32 devices in a mesh: scene: 2 (over x), az: 16 (over z, y, core).
Axes of the slice: x: 2, y: 2, z: 4, core: 2. Of those that a mesh axis runs over, the one named last changes fastest.
Arguments:
- secondary: bfloat16 [2, 512, 12288], P(None, ('scene', 'az')), parts along dimension 1, may hold values from -6 to 6
- line_valid: int32 [512], P(('scene', 'az')), parts along dimension 0, may hold values 0 or 1
- first_valid: int32 [512], P(('scene', 'az')), parts along dimension 0, may hold values from 0 to 3071
- last_valid: int32 [512], P(('scene', 'az')), parts along dimension 0, may hold values from 9216 to 12288
- az_coef: float32 [3, 512], P(None, ('scene', 'az')), parts along dimension 1, may hold values from -0.33 to 0.33
- az_base: int32 [512], P(('scene', 'az')), parts along dimension 0, may hold values from -3 to 3
- rg_base: int32 [512], P(('scene', 'az')), parts along dimension 0, may hold values from -8 to 8
- rg_coef: float32 [8], P('scene'), parts along dimension 0, may hold values from -3 to 3
- block_dest: int32 [512], P(('scene', 'az')), parts along dimension 0, may hold values from 0 to 255, as said below
Outputs:
- coreg: bfloat16 [2, 512, 12288], P(None, ('scene', 'az')), parts along dimension 1
- mean_power: float32 [2], P('scene'), parts along dimension 0
- valid_share: float32 [2], P('scene'), parts along dimension 0
The draws below stay inside these ranges and needn't reach their ends.
There are 2 independent parts, one for each index of `scene`. The reference program is written for one: setup_inputs(seed, part) draws one part's arguments, and reference() takes and returns one part's arrays. A program takes and returns all parts, laid end to end along the dimension named above; each array names one. Nothing has to cross between parts.
Inputs may be any that keep to these rules, and one draw needn't show every extreme that they name: `block_dest`: A permutation of 0 to 255. The 16 line blocks of each device of az take exactly one place on every device of az, itself included (place // 16 runs over all devices).
All inputs are finite; a program needn't handle non-finite values. No bound on the sum of `line_valid` on one device may be relied on, other than what follows from the above.
Results may differ from the reference program's by a relative error of at most 0.0066.
Values may be sent and summed in bfloat16 or wider, within the bound.
A program may use at most 128 MiB of HBM per device.

```python
import jax
import jax.numpy as jnp
from jax import lax

LINES = 1
RG = 12288
ABASE = 3
RBMAX = 8
HALO = 7
BLK_DEV = 16
AZ = 256
NBLK = 256


def draw_secondary(key, part):
    first_key, second_key = jax.random.split(key)
    values = jax.random.normal(first_key, (2, AZ, RG), jnp.float32)
    return jnp.clip(values, -6.0, 6.0).astype(jnp.bfloat16)


def draw_block_dest(key, part):
    blocks = BLK_DEV
    first_key, second_key = jax.random.split(key)
    offsets = jax.vmap(lambda inner_key: jax.random.permutation(inner_key, blocks))(jax.random.split(first_key, blocks))
    places = jax.vmap(lambda inner_key: jax.random.permutation(inner_key, blocks))(jax.random.split(second_key, blocks))
    source = jnp.broadcast_to(jnp.arange(blocks)[:, None], (blocks, blocks))
    target = (source + offsets) % blocks
    slot_at = places[target, source]
    return (target * blocks + slot_at).reshape(-1).astype(jnp.int32)


def touch_ends(array, stream_key, least, top_value):
    dims = array.shape
    index_at = [jax.random.randint(jax.random.fold_in(stream_key, axis), (), 0, dims[axis]) for axis in range(len(dims))]
    array = array.at[tuple(index_at)].set(least)
    longest = dims.index(max(dims))
    index_at[longest] = (index_at[longest] + 1) % dims[longest]
    return array.at[tuple(index_at)].set(top_value)


def block_levels(own_key, dims, cuts, low, largest):
    factor_of, own = 1.0, jax.random.fold_in(own_key, 6)
    for dim, parts in cuts:
        draws = jnp.exp(jax.random.uniform(jax.random.fold_in(own, dim), (parts,), jnp.float32, low / len(cuts), largest / len(cuts)))
        factor_of = factor_of * jnp.repeat(draws, dims[dim] // parts).reshape([-1 if axis == dim else 1 for axis in range(len(dims))])
    return factor_of


def setup_inputs(seed: int = 0, part: int = 0) -> dict:
    key_list = jax.random.split(jax.random.key(seed), 10)
    own_keys = jax.random.split(jax.random.fold_in(key_list[9], part), 10)
    return {
        "secondary": draw_secondary(jax.random.fold_in(jax.random.fold_in(key_list[9], part), 71), part),
        "line_valid": touch_ends((jax.random.randint(own_keys[1], (AZ,), 0, 4) < 3).astype(jnp.int32), jax.random.fold_in(own_keys[1], 1), 0, 1),
        "first_valid": touch_ends(jax.random.randint(own_keys[2], (AZ,), 0, RG // 4), jax.random.fold_in(own_keys[2], 1), 0, (RG // 4) - 1).astype(jnp.int32),
        "last_valid": touch_ends(jax.random.randint(own_keys[3], (AZ,), RG - RG // 4, RG + 1), jax.random.fold_in(own_keys[3], 1), RG - RG // 4, RG).astype(jnp.int32),
        "az_coef": jnp.clip(jax.random.uniform(own_keys[4], (3, NBLK), jnp.float32, -0.33, 0.33) * block_levels(own_keys[4], (3, NBLK), ((1, 16),), -0.4, 0.0), -0.33, 0.33),
        "az_base": touch_ends(jax.random.randint(own_keys[5], (NBLK,), -ABASE, ABASE + 1), jax.random.fold_in(own_keys[5], 1), -ABASE, ABASE).astype(jnp.int32),
        "rg_base": touch_ends(jax.random.randint(own_keys[6], (NBLK,), -RBMAX, RBMAX + 1), jax.random.fold_in(own_keys[6], 1), -RBMAX, RBMAX).astype(jnp.int32),
        "rg_coef": jnp.clip(jax.random.uniform(own_keys[7], (4,), jnp.float32, -3.0, 3.0), -3.0, 3.0),
        "block_dest": draw_block_dest(jax.random.fold_in(jax.random.fold_in(key_list[9], part), 71), part),
    }


def sinc_taper(distance):
    in_reach = jnp.abs(distance) < 4.0
    shaped = jnp.sinc(distance) * (0.5 + 0.5 * jnp.cos(jnp.pi * distance / 4.0))
    return jnp.where(in_reach, shaped, jnp.zeros_like(distance))

def tap_weights(az_coef, line_count):
    position = (jnp.arange(line_count, dtype=jnp.float32) + 0.5) / line_count
    fraction = az_coef[0][:, None] + az_coef[1][:, None] * position + az_coef[2][:, None] * position * position
    tap_offsets = jnp.arange(9, dtype=jnp.float32) - 4.0
    return sinc_taper(tap_offsets[None, None, :] - fraction[:, :, None]).astype(jnp.bfloat16)

def range_tiles(rg_coef, col_count):
    tile_total = col_count // 128
    col_index = jnp.arange(col_count, dtype=jnp.float32)
    along = (col_index + 0.5) / col_count
    offsets = rg_coef[0] + rg_coef[1] * along + rg_coef[2] * along * along + rg_coef[3] * along * along * along
    offsets = offsets.reshape(tile_total, 128)
    inner = jnp.arange(128, dtype=jnp.float32)
    tile_gaps = (jnp.arange(3, dtype=jnp.float32) - 1.0) * 128.0
    distance = tile_gaps[:, None, None, None] + inner[None, None, :, None] - inner[None, None, None, :] - offsets[None, :, None, :]
    return sinc_taper(distance).astype(jnp.bfloat16)

def resample(windows, weights, kernel):
    line_count = weights.shape[1]
    summed = jnp.zeros(windows.shape[:2] + (line_count, windows.shape[3]), jnp.float32)
    for tap_index in range(9):
        summed = summed + weights[:, None, :, tap_index, None].astype(jnp.float32) * windows[:, :, tap_index:tap_index + line_count, :].astype(jnp.float32)
    azimuthal = summed.astype(jnp.bfloat16)
    col_count = azimuthal.shape[3]
    tile_total = col_count // 128
    tiled_rows = azimuthal.reshape(azimuthal.shape[:3] + (tile_total, 128))
    padded = jnp.pad(tiled_rows, ((0, 0), (0, 0), (0, 0), (1, 1), (0, 0)))
    ranged = jnp.zeros(tiled_rows.shape, jnp.float32)
    for shift_tile in range(3):
        ranged = ranged + jnp.einsum('bclti,tij->bcltj', padded[:, :, :, shift_tile:shift_tile + tile_total].astype(jnp.float32), kernel[shift_tile].astype(jnp.float32))
    return ranged.reshape(azimuthal.shape).astype(jnp.bfloat16)

def reference(secondary, line_valid, first_valid, last_valid, az_coef, az_base, rg_base, rg_coef, block_dest):
    col_index = jnp.arange(RG, dtype=jnp.int32)
    kept_mask = (line_valid[:, None] > 0) & (col_index[None, :] >= first_valid[:, None]) & (col_index[None, :] < last_valid[:, None])
    masked = jnp.where(kept_mask[None], secondary, jnp.zeros((), jnp.bfloat16))
    valid_total = jnp.sum(kept_mask.astype(jnp.int32)).astype(jnp.float32)
    padded = jnp.pad(masked, ((0, 0), (HALO, HALO), (RBMAX, RBMAX)))
    weights = tap_weights(az_coef, LINES)
    kernel = range_tiles(rg_coef, RG)
    row_starts = (jnp.arange(NBLK, dtype=jnp.int32) * LINES + az_base - 4 + HALO).astype(jnp.int32)
    col_starts = (RBMAX + rg_base).astype(jnp.int32)

    def one_group(group_index):
        first_block = (group_index * BLK_DEV).astype(jnp.int32)
        rows_here = lax.dynamic_slice_in_dim(row_starts, first_block, BLK_DEV)
        cols_here = lax.dynamic_slice_in_dim(col_starts, first_block, BLK_DEV)
        windows = jax.vmap(lambda rows_at, cols_at: lax.dynamic_slice(padded, (jnp.int32(0), rows_at, cols_at), (2, LINES + 8, RG)))(rows_here, cols_here)
        group_weights = lax.dynamic_slice_in_dim(weights, first_block, BLK_DEV)
        return resample(windows, group_weights, kernel)
    resampled_groups = lax.map(one_group, jnp.arange(NBLK // BLK_DEV, dtype=jnp.int32))
    resampled = resampled_groups.reshape(NBLK, 2, LINES, RG)
    total_power = jnp.sum(jnp.square(resampled.astype(jnp.float32)))
    mean_power = total_power / jnp.maximum(valid_total, 1.0)
    power_gain = lax.rsqrt(mean_power + 0.5)
    scaled = (resampled.astype(jnp.float32) * power_gain).astype(jnp.bfloat16)
    placed = jnp.zeros_like(scaled).at[block_dest].set(scaled)
    coreg = jnp.moveaxis(placed, 1, 0).reshape(2, AZ, RG)
    valid_share = valid_total / (AZ * RG)
    return (coreg, mean_power.reshape(1), valid_share.reshape(1))
```

```python
import functools

import jax
import jax.numpy as jnp
from jax import lax
from jax.experimental import pallas as pl
from jax.experimental.pallas import tpu as pltpu
from jax.sharding import PartitionSpec as P

HALO = 8
TAPS = 11
NOTE = 8
PI = 3.141592653589793
HALF = 0.7071067811865476
COS8 = (1.0, HALF, 0.0, -HALF, -1.0, -HALF, 0.0, HALF)


def range_weights(coef, start, weight, cols):
    for g in range(cols // 1024):
        centre = (g * 1024 + 512) / cols
        oc = coef[0] + coef[1] * centre + coef[2] * (centre * centre) + coef[3] * (centre**3)
        n0 = (oc - 5.0 + 64.0).astype(jnp.int32) - 63
        start[g] = n0
        sub = lax.broadcasted_iota(jnp.int32, (8, 128), 0)
        lane = lax.broadcasted_iota(jnp.int32, (8, 128), 1)
        col = g * 1024 + sub * 128 + lane
        v = (col.astype(jnp.float32) + 0.5) / cols
        off = coef[0] + coef[1] * v + coef[2] * v * v + coef[3] * v * v * v
        whole = jnp.round(off)
        part = off - whole
        odd = (whole.astype(jnp.int32) + n0) & 1
        sine = jnp.sin(PI * part) * (-1.0 / PI) * (1 - 2 * odd).astype(jnp.float32)
        base = (n0.astype(jnp.float32) - off) * (PI / 4.0)
        c0, s0 = jnp.cos(base), jnp.sin(base)
        for k in range(TAPS):
            n = n0 + k
            d = n.astype(jnp.float32) - off
            ck, sk = COS8[k % 8], COS8[(k - 2) % 8]
            taper = 0.5 + 0.5 * (c0 * ck - s0 * sk)
            top = sine if k % 2 == 0 else -sine
            near = d == 0.0
            val = jnp.where(near, 1.0, top / jnp.where(near, 1.0, d)) * taper
            keep = (jnp.abs(d) < 4.0) & (col + n >= 0) & (col + n < cols)
            val = jnp.where(keep, val, 0.0)
            weight[g, k] = val.astype(jnp.bfloat16).astype(jnp.float32)


def column(values):
    row = lax.broadcasted_iota(jnp.int32, (len(values), 128), 0)
    made = jnp.zeros((len(values), 128), jnp.asarray(values[0]).dtype)
    for r, value in enumerate(values):
        made = jnp.where(row == r, value, made)
    return made


def azimuth_band(fraction, base, line, blocks):
    held = lax.broadcasted_iota(jnp.int32, (blocks, 128), 1)
    row = jnp.where(held < blocks, held, held - blocks - HALO)
    row = jnp.where(held < blocks + HALO, row, held - HALO)
    gap = row - line - base
    d = gap.astype(jnp.float32) - fraction
    near = d == 0.0
    safe = jnp.where(near, 1.0, d)
    whole = jnp.round(safe)
    sine = jnp.sin(PI * (safe - whole)) * (1 - 2 * (whole.astype(jnp.int32) & 1)).astype(jnp.float32)
    value = jnp.where(near, 1.0, sine / (PI * safe)) * (0.5 + 0.5 * jnp.cos(PI * d / 4.0))
    keep = (jnp.abs(d) < 4.0) & (jnp.abs(gap) <= 4) & (held < blocks + 2 * HALO)
    return jnp.where(keep, value, 0.0).astype(jnp.bfloat16)


def send_order(me, count, i):
    half = count // 2
    mine = me // half
    own = i // half
    side = mine * own + (1 - mine) * (1 - own)
    return side * half + lax.rem(me - mine * half + own + i - own * half, half)


def swath_kernel(
    cuts, coef_in, shift_in, dest_in, valid_in, first_in, last_in, az_coef_in, az_base_in, image,
    nat, notes,
    coef, shift, dest, valid, first, last, az_coef, az_base,
    held, edge, dense, weight, sent, got, memo, start, order,
    ready, load_sem, own_sem, halo_send, halo_recv, edge_send, edge_recv, send_sem, recv_sem, note_send, note_recv,
):
    blocks, cols = image.shape[1], image.shape[2]
    tiles = cols // 128
    span = dense.shape[0] // (2 * blocks)
    count = lax.axis_size("az")
    me = lax.axis_index("az")
    after, before = lax.rem(me + 1, count), lax.rem(me + count - 1, count)
    up, down = me < count - 1, me > 0

    barrier = pltpu.get_barrier_semaphore()
    near = min(NEAR, count - 1)

    def greet(semaphore, step):
        @pl.when(me + step < count)
        def _():
            pl.semaphore_signal(semaphore, inc=1, device_id={"az": lax.rem(me + step, count)})

        @pl.when(me >= step)
        def _():
            pl.semaphore_signal(semaphore, inc=1, device_id={"az": lax.rem(me + count - step, count)})

    for step in range(1, near + 1):
        greet(barrier, step)
    own = pltpu.make_async_copy(image, held.at[:, pl.ds(0, blocks)], own_sem)
    own.start()
    loads = [
        pltpu.make_async_copy(source, target, load_sem.at[k])
        for k, (source, target) in enumerate(
            (
                (valid_in, valid), (first_in, first), (last_in, last), (coef_in, coef),
                (shift_in, shift), (dest_in, dest), (az_coef_in, az_coef), (az_base_in, az_base),
            )
        )
    ]
    for load in loads:
        load.start()
    for load in loads:
        load.wait()
    low_edge = [jnp.where(valid[r] > 0, first[r], cols) for r in range(blocks)]
    high_edge = [jnp.where(valid[r] > 0, last[r], 0) for r in range(blocks)]
    edge[0, pl.ds(0, blocks), :] = column(low_edge).astype(jnp.float32)
    edge[1, pl.ds(0, blocks), :] = column(high_edge).astype(jnp.float32)
    own.wait()
    pl.semaphore_wait(barrier, jnp.minimum(me, near) + jnp.minimum(count - 1 - me, near))

    chunks = len(cuts) - 1
    bounds = [0] + [cut * 16 + 1 for cut in cuts[1:-1]] + [tiles]
    ways = ((after, blocks - HALO, blocks, up, down), (before, 0, blocks + HALO, down, up))

    def begin(copy, sends):
        @pl.when(sends)
        def _():
            copy.start()

    def finish(copy, sends, receives):
        @pl.when(sends)
        def _():
            copy.wait_send()

        @pl.when(receives)
        def _():
            copy.wait_recv()

    halo = []
    for c in range(chunks):
        at = pl.ds(bounds[c] * 128, (bounds[c + 1] - bounds[c]) * 128)
        for w, (peer, source, slot, sends, receives) in enumerate(ways):
            copy = pltpu.make_async_remote_copy(
                src_ref=held.at[:, pl.ds(source, HALO), at],
                dst_ref=held.at[:, pl.ds(slot, HALO), at],
                send_sem=halo_send.at[c, w],
                recv_sem=halo_recv.at[c, w],
                device_id={"az": peer},
            )
            begin(copy, sends)
            halo.append((copy, sends, receives))
        if c == 0:
            bounds_sent = []
            for w, (peer, source, slot, sends, receives) in enumerate(ways):
                copy = pltpu.make_async_remote_copy(
                    src_ref=edge.at[:, pl.ds(source, HALO), :],
                    dst_ref=edge.at[:, pl.ds(slot, HALO), :],
                    send_sem=edge_send.at[w],
                    recv_sem=edge_recv.at[w],
                    device_id={"az": peer},
                )
                begin(copy, sends)
                bounds_sent.append((copy, sends, receives))

    reach = near
    stage = 0
    if reach < count - 1:
        greet(ready.at[0], reach)

    lines = []
    for i in range(blocks):
        target = send_order(me, count, i)
        line = jnp.int32(0)
        for j in range(blocks):
            line = jnp.where(dest[j] // blocks == target, j, line)
        order[i] = line
        lines.append(line)
    c0 = column([az_coef[0, j] for j in lines])
    c1 = column([az_coef[1, j] for j in lines])
    c2 = column([az_coef[2, j] for j in lines])
    q = 0.5
    fraction = c0 + c1 * q + c2 * q * q
    band = azimuth_band(fraction, column([az_base[j] for j in lines]), column(lines), blocks)
    band = band[:, : blocks + 2 * HALO]
    range_weights(coef, start, weight, cols)
    while reach < count - 1:
        pl.semaphore_wait(
            ready.at[stage], (me >= reach).astype(jnp.int32) + (me + reach < count).astype(jnp.int32)
        )
        reach, stage = 2 * reach, stage + 1
        if reach < count - 1:
            greet(ready.at[stage], reach)

    for copy, sends, receives in bounds_sent:
        finish(copy, sends, receives)
    low = edge[0]
    high = edge[1]
    row = lax.broadcasted_iota(jnp.int32, high.shape, 0)
    outside = ((me == 0) & (row >= blocks) & (row < blocks + HALO)) | (
        (me == count - 1) & (row >= blocks + HALO)
    )
    high = jnp.where(outside, 0.0, high)
    lane_held = lax.broadcasted_iota(jnp.int32, high.shape, 1).astype(jnp.float32)
    lane_row = lax.broadcasted_iota(jnp.int32, (blocks, 128), 1)
    lane = lax.broadcasted_iota(jnp.int32, (8, 128), 1)

    def azimuth(first_tile, wide, tails):
        at = pl.ds(first_tile * 128, wide * 128)
        keeps = []
        for u in range(wide):
            col = lane_held + ((first_tile + u) * 128.0)
            keeps.append((col >= low) & (col < high))
        new_tails = []
        for p in range(2):
            rows = held[p, :, at].astype(jnp.float32)
            rows = jnp.concatenate(
                [
                    jnp.where(keep, rows[:, u * 128 : u * 128 + 128], 0.0)
                    for u, keep in enumerate(keeps)
                ],
                axis=1,
            ).astype(jnp.bfloat16)
            out = jnp.dot(band, rows, preferred_element_type=jnp.float32)
            out = out.astype(jnp.bfloat16).astype(jnp.float32)
            tail = tails[p]
            for u in range(wide):
                turned = pltpu.roll(out[:, u * 128 : u * 128 + 128], 64, 1)
                place = p * blocks * span + first_tile + u
                dense[pl.ds(place, blocks, stride=span), :] = jnp.where(lane_row < 64, tail, turned)
                tail = turned
            new_tails.append(tail)
        return tuple(new_tails)

    def filtered(i, big, power):
        for p in range(2):
            halves = []
            for h in range(2):
                g = big * 2 + h
                b = shift[order[i]] + start[g] + 64
                at = pl.multiple_of((p * blocks + i) * span + g * 8, 8)
                x0 = dense[pl.ds(at, 8), :]
                x1 = dense[pl.ds(at + 1, 8), :]
                acc = None
                for k in range(TAPS):
                    moved = pltpu.roll(jnp.where(lane < b + k, x1, x0), 128 - b - k, 1)
                    term = weight[g, k] * moved
                    acc = term if acc is None else acc + term
                halves.append(acc)
            done = jnp.concatenate(halves, axis=0).astype(jnp.bfloat16)
            sent[i, p, pl.ds(pl.multiple_of(big * 16, 16), 16), :] = done
            wide = done.astype(jnp.float32)
            power = power + wide * wide
        return power

    def parcel(c, i):
        at = pl.ds(cuts[c] * 16, (cuts[c + 1] - cuts[c]) * 16)
        peer = send_order(me, count, i)
        return pltpu.make_async_remote_copy(
            src_ref=sent.at[i, :, at, :],
            dst_ref=got.at[me, :, at, :],
            send_sem=send_sem.at[c, i],
            recv_sem=recv_sem.at[c, me],
            device_id={"az": peer},
        )

    tails = (jnp.zeros((blocks, 128), jnp.float32),) * 2
    power = jnp.zeros((16, 128), jnp.float32)
    for c in range(chunks):
        for copy, sends, receives in halo[2 * c : 2 * c + 2]:
            finish(copy, sends, receives)
        for first_tile in range(bounds[c], bounds[c + 1], WIDE):
            tails = azimuth(first_tile, min(WIDE, bounds[c + 1] - first_tile), tails)
        if c == chunks - 1:
            for p in range(2):
                ends = jnp.where(lane_row < 64, tails[p], 0.0)
                dense[pl.ds(p * blocks * span + tiles, blocks, stride=span), :] = ends
        lo, hi = cuts[c], cuts[c + 1]

        def line(i, power):
            power = lax.fori_loop(lo, hi, functools.partial(filtered, i), power, unroll=True)
            if c < chunks - 1:

                @pl.when(i < count - 1)
                def _():
                    parcel(c, i).start()

            return power

        power = lax.fori_loop(0, blocks, line, power)

    own_power = jnp.broadcast_to(jnp.sum(power, keepdims=True), (1, 128))
    have = jnp.int32(0)
    for j in range(blocks):
        have = have + jnp.maximum(
            jnp.minimum(high_edge[j], cols) - jnp.maximum(low_edge[j], 0), 0
        )
    own_count = jnp.full((1, 128), have, jnp.int32).astype(jnp.float32)
    lane_note = lax.broadcasted_iota(jnp.int32, (1, 128), 1)
    stats = jnp.where(lane_note == 127, own_power, own_count)
    for i in range(blocks):
        place = jnp.full((1, 128), dest[lines[i]] % blocks, jnp.int32).astype(jnp.float32)
        memo[i] = jnp.where(lane_note < 126, place, stats)

    def told(i):
        return pltpu.make_async_remote_copy(
            src_ref=memo.at[i],
            dst_ref=notes.at[me],
            send_sem=note_send.at[i],
            recv_sem=note_recv.at[me],
            device_id={"az": send_order(me, count, i)},
        )

    def tell(i, carry):
        told(i).start()
        return carry

    def last_send(i, carry):
        parcel(chunks - 1, i).start()
        return carry

    lax.fori_loop(0, count - 1, tell, 0)
    lax.fori_loop(0, count - 1, last_send, 0)
    notes[me] = memo[blocks - 1]
    got[me] = sent[blocks - 1]

    for c in range(chunks):
        lo, wide = cuts[c] * 16, (cuts[c + 1] - cuts[c]) * 16
        at = pl.ds(lo, wide)

        def take(i, carry):
            peer = send_order(me, count, i)
            parcel(c, i).wait_send()
            pltpu.make_async_remote_copy(
                src_ref=sent.at[i, :, at, :],
                dst_ref=got.at[peer, :, at, :],
                send_sem=send_sem.at[c, i],
                recv_sem=recv_sem.at[c, peer],
                device_id={"az": peer},
            ).wait_recv()
            return carry

        lax.fori_loop(0, count - 1, take, 0)

        def spread(s, carry):
            for p in range(2):
                dense[pl.ds((p * blocks + s) * span + lo, wide), :] = got[s, p, at, :].astype(jnp.float32)
            return carry

        lax.fori_loop(0, blocks, spread, 0)
        for t in range(lo, lo + wide):
            for p in range(2):
                x = dense[pl.ds(p * blocks * span + t, blocks, stride=span), :]
                nat[p, :, t * 128 : t * 128 + 128] = x.astype(jnp.bfloat16)

    def hear(i, carry):
        peer = send_order(me, count, i)
        told(i).wait_send()
        pltpu.make_async_remote_copy(
            src_ref=memo.at[i],
            dst_ref=notes.at[peer],
            send_sem=note_send.at[i],
            recv_sem=note_recv.at[peer],
            device_id={"az": peer},
        ).wait_recv()
        return carry

    lax.fori_loop(0, count - 1, hear, 0)


def finish_kernel(total, nat, notes, out, mean, share):
    blocks, cols = out.shape[1], out.shape[2]
    told = [notes[s] for s in range(blocks)]
    both = functools.reduce(lambda a, b: a + b, told)
    power, count = both[:, 127:128], both[:, 126:127]
    mean_power = power / jnp.maximum(count, 1.0)
    gain = lax.rsqrt(mean_power + 0.5)
    lane = lax.broadcasted_iota(jnp.int32, (1, 128), 1)
    place = functools.reduce(
        lambda a, s: jnp.where(lane == s, told[s], a), range(blocks), jnp.full((1, 128), -1.0)
    )
    row = lax.broadcasted_iota(jnp.int32, (blocks, 128), 0).astype(jnp.float32)
    pick = (row == place).astype(jnp.float32).astype(jnp.bfloat16)[:, :blocks]
    for p in range(2):
        for t in range(0, cols, 1024):
            wide = min(1024, cols - t)
            x = jnp.dot(pick, nat[p, :, t : t + wide], preferred_element_type=jnp.float32)
            out[p, :, t : t + wide] = (x * gain).astype(jnp.bfloat16)
    mean[0] = mean_power[0, 0]
    share[0] = (count / float(total))[0, 0]


def shards(
    secondary, line_valid, first_valid, last_valid, az_coef, az_base, rg_base, rg_coef, block_dest
):
    cols = secondary.shape[2]
    blocks = block_dest.shape[0]
    tiles = cols // 128
    count = lax.axis_size("az")
    bigs = tiles // 16
    cuts = [0] + sorted({bigs * cut // 6 for cut in CUTS} - {0, bigs}) + [bigs]
    chunks = len(cuts) - 1
    parts = max(c for c in range(1, PARTS + 1) if bigs % c == 0)
    vmem = pl.BlockSpec(memory_space=pltpu.VMEM)
    smem = pl.BlockSpec(memory_space=pltpu.SMEM)
    held = blocks + 2 * HALO
    dma = pltpu.SemaphoreType.DMA
    stages = max(1, (-(-count // NEAR)).bit_length())
    nat, notes = pl.pallas_call(
        functools.partial(swath_kernel, cuts),
        out_shape=(
            jax.ShapeDtypeStruct((2, blocks, cols), jnp.bfloat16),
            jax.ShapeDtypeStruct((blocks, 1, 128), jnp.float32),
        ),
        in_specs=[pl.BlockSpec(memory_space=pl.ANY)] * 9,
        out_specs=(vmem, vmem),
        scratch_shapes=[
            pltpu.SMEM(rg_coef.shape, jnp.float32),
            pltpu.SMEM((blocks,), jnp.int32),
            pltpu.SMEM((blocks,), jnp.int32),
            pltpu.SMEM((blocks,), jnp.int32),
            pltpu.SMEM((blocks,), jnp.int32),
            pltpu.SMEM((blocks,), jnp.int32),
            pltpu.SMEM(az_coef.shape, jnp.float32),
            pltpu.SMEM((blocks,), jnp.int32),
            pltpu.VMEM((2, held, cols), jnp.bfloat16),
            pltpu.VMEM((2, held, 128), jnp.float32),
            pltpu.VMEM((2 * blocks * (tiles + 8), 128), jnp.float32),
            pltpu.VMEM((tiles // 8, TAPS, 8, 128), jnp.float32),
            pltpu.VMEM((blocks, 2, tiles, 128), jnp.bfloat16),
            pltpu.VMEM((blocks, 2, tiles, 128), jnp.bfloat16),
            pltpu.VMEM((blocks, 1, 128), jnp.float32),
            pltpu.SMEM((tiles // 8,), jnp.int32),
            pltpu.SMEM((blocks,), jnp.int32),
            pltpu.SemaphoreType.REGULAR((stages,)),
            dma((8,)),
            dma(()),
            dma((chunks, 2)),
            dma((chunks, 2)),
            dma((2,)),
            dma((2,)),
            dma((chunks, blocks)),
            dma((chunks, blocks)),
            dma((blocks,)),
            dma((blocks,)),
        ],
        compiler_params=pltpu.CompilerParams(collective_id=0, has_side_effects=True),
        name="swath",
    )(
        rg_coef, rg_base, block_dest, line_valid, first_valid, last_valid, az_coef, az_base,
        secondary,
    )
    return pl.pallas_call(
        functools.partial(finish_kernel, cols * blocks * count),
        out_shape=(
            jax.ShapeDtypeStruct((2, blocks, cols), jnp.bfloat16),
            jax.ShapeDtypeStruct((1,), jnp.float32),
            jax.ShapeDtypeStruct((1,), jnp.float32),
        ),
        grid=(parts,),
        in_specs=[pl.BlockSpec((2, blocks, cols // parts), lambda c: (0, 0, c)), vmem],
        out_specs=(pl.BlockSpec((2, blocks, cols // parts), lambda c: (0, 0, c)), smem, smem),
        name="finish",
    )(nat, notes)


CUTS = (1, 3)
PARTS = 2
NEAR = 4
WIDE = 9


def solution(mesh):
    rows = P(("scene", "az"))
    placed = (
        P(None, ("scene", "az"), None),
        rows,
        rows,
        rows,
        P(None, ("scene", "az")),
        rows,
        rows,
        P("scene"),
        rows,
    )
    return jax.shard_map(
        shards,
        mesh=mesh,
        in_specs=placed,
        out_specs=(P(None, ("scene", "az"), None), P("scene"), P("scene")),
        check_vma=False,
    )
```

```python
import functools

import jax
import jax.numpy as jnp
from jax import lax
from jax.experimental import pallas as pl
from jax.experimental.pallas import tpu as pltpu
from jax.sharding import PartitionSpec as P

HALO = 8
TAPS = 11
NOTE = 8
PI = 3.141592653589793
HALF = 0.7071067811865476
COS8 = (1.0, HALF, 0.0, -HALF, -1.0, -HALF, 0.0, HALF)


def range_weights(coef, start, weight, cols):
    for g in range(cols // 1024):
        centre = (g * 1024 + 512) / cols
        oc = coef[0] + coef[1] * centre + coef[2] * (centre * centre) + coef[3] * (centre**3)
        n0 = (oc - 5.0 + 64.0).astype(jnp.int32) - 63
        start[g] = n0
        sub = lax.broadcasted_iota(jnp.int32, (8, 128), 0)
        lane = lax.broadcasted_iota(jnp.int32, (8, 128), 1)
        col = g * 1024 + sub * 128 + lane
        v = (col.astype(jnp.float32) + 0.5) / cols
        off = coef[0] + coef[1] * v + coef[2] * v * v + coef[3] * v * v * v
        whole = jnp.round(off)
        part = off - whole
        odd = (whole.astype(jnp.int32) + n0) & 1
        sine = jnp.sin(PI * part) * (-1.0 / PI) * (1 - 2 * odd).astype(jnp.float32)
        base = (n0.astype(jnp.float32) - off) * (PI / 4.0)
        c0, s0 = jnp.cos(base), jnp.sin(base)
        for k in range(TAPS):
            n = n0 + k
            d = n.astype(jnp.float32) - off
            ck, sk = COS8[k % 8], COS8[(k - 2) % 8]
            taper = 0.5 + 0.5 * (c0 * ck - s0 * sk)
            top = sine if k % 2 == 0 else -sine
            near = d == 0.0
            val = jnp.where(near, 1.0, top / jnp.where(near, 1.0, d)) * taper
            keep = (jnp.abs(d) < 4.0) & (col + n >= 0) & (col + n < cols)
            val = jnp.where(keep, val, 0.0)
            weight[g, k] = val.astype(jnp.bfloat16).astype(jnp.float32)


def column(values):
    row = lax.broadcasted_iota(jnp.int32, (len(values), 128), 0)
    made = jnp.zeros((len(values), 128), jnp.asarray(values[0]).dtype)
    for r, value in enumerate(values):
        made = jnp.where(row == r, value, made)
    return made


def azimuth_band(fraction, base, line, blocks):
    held = lax.broadcasted_iota(jnp.int32, (blocks, 128), 1)
    row = jnp.where(held < blocks, held, held - blocks - HALO)
    row = jnp.where(held < blocks + HALO, row, held - HALO)
    gap = row - line - base
    d = gap.astype(jnp.float32) - fraction
    near = d == 0.0
    safe = jnp.where(near, 1.0, d)
    whole = jnp.round(safe)
    sine = jnp.sin(PI * (safe - whole)) * (1 - 2 * (whole.astype(jnp.int32) & 1)).astype(jnp.float32)
    value = jnp.where(near, 1.0, sine / (PI * safe)) * (0.5 + 0.5 * jnp.cos(PI * d / 4.0))
    keep = (jnp.abs(d) < 4.0) & (jnp.abs(gap) <= 4) & (held < blocks + 2 * HALO)
    return jnp.where(keep, value, 0.0).astype(jnp.bfloat16)


def send_order(me, count, i):
    half = count // 2
    mine = me // half
    own = i // half
    side = mine * own + (1 - mine) * (1 - own)
    near = lax.rem(me - mine * half + own + i - own * half, half)
    if half % 2:
        return side * half + near
    quarter = half // 2
    group = i // quarter
    far = (mine * group + (1 - mine) * (1 - group)) * quarter + lax.rem(me + i, quarter)
    return side * half + jnp.where(own == 1, near, far)


def swath_kernel(
    cuts, coef_in, shift_in, dest_in, valid_in, first_in, last_in, az_coef_in, az_base_in, image,
    nat, notes,
    coef, shift, dest, valid, first, last, az_coef, az_base,
    held, edge, dense, weight, sent, got, memo, start, order,
    ready, load_sem, own_sem, halo_send, halo_recv, edge_send, edge_recv, send_sem, recv_sem, note_send, note_recv,
):
    blocks, cols = image.shape[1], image.shape[2]
    tiles = cols // 128
    span = dense.shape[0] // (2 * blocks)
    count = lax.axis_size("az")
    me = lax.axis_index("az")
    after, before = lax.rem(me + 1, count), lax.rem(me + count - 1, count)
    up, down = me < count - 1, me > 0

    barrier = pltpu.get_barrier_semaphore()
    near = min(NEAR, count - 1)

    def greet(semaphore, step):
        @pl.when(me + step < count)
        def _():
            pl.semaphore_signal(semaphore, inc=1, device_id={"az": lax.rem(me + step, count)})

        @pl.when(me >= step)
        def _():
            pl.semaphore_signal(semaphore, inc=1, device_id={"az": lax.rem(me + count - step, count)})

    for step in range(1, near + 1):
        greet(barrier, step)
    own = pltpu.make_async_copy(image, held.at[:, pl.ds(0, blocks)], own_sem)
    own.start()
    loads = [
        pltpu.make_async_copy(source, target, load_sem.at[k])
        for k, (source, target) in enumerate(
            (
                (valid_in, valid), (first_in, first), (last_in, last), (coef_in, coef),
                (shift_in, shift), (dest_in, dest), (az_coef_in, az_coef), (az_base_in, az_base),
            )
        )
    ]
    for load in loads:
        load.start()
    for load in loads:
        load.wait()
    low_edge = [jnp.where(valid[r] > 0, first[r], cols) for r in range(blocks)]
    high_edge = [jnp.where(valid[r] > 0, last[r], 0) for r in range(blocks)]
    edge[0, pl.ds(0, blocks), :] = column(low_edge).astype(jnp.float32)
    edge[1, pl.ds(0, blocks), :] = column(high_edge).astype(jnp.float32)
    own.wait()
    pl.semaphore_wait(barrier, jnp.minimum(me, near) + jnp.minimum(count - 1 - me, near))

    chunks = len(cuts) - 1
    bounds = [0] + [cut * 16 + 1 for cut in cuts[1:-1]] + [tiles]
    ways = ((after, blocks - HALO, blocks, up, down), (before, 0, blocks + HALO, down, up))

    def begin(copy, sends):
        @pl.when(sends)
        def _():
            copy.start()

    def finish(copy, sends, receives):
        @pl.when(sends)
        def _():
            copy.wait_send()

        @pl.when(receives)
        def _():
            copy.wait_recv()

    halo = []
    for c in range(chunks):
        at = pl.ds(bounds[c] * 128, (bounds[c + 1] - bounds[c]) * 128)
        for w, (peer, source, slot, sends, receives) in enumerate(ways):
            copy = pltpu.make_async_remote_copy(
                src_ref=held.at[:, pl.ds(source, HALO), at],
                dst_ref=held.at[:, pl.ds(slot, HALO), at],
                send_sem=halo_send.at[c, w],
                recv_sem=halo_recv.at[c, w],
                device_id={"az": peer},
            )
            begin(copy, sends)
            halo.append((copy, sends, receives))
        if c == 0:
            bounds_sent = []
            for w, (peer, source, slot, sends, receives) in enumerate(ways):
                copy = pltpu.make_async_remote_copy(
                    src_ref=edge.at[:, pl.ds(source, HALO), :],
                    dst_ref=edge.at[:, pl.ds(slot, HALO), :],
                    send_sem=edge_send.at[w],
                    recv_sem=edge_recv.at[w],
                    device_id={"az": peer},
                )
                begin(copy, sends)
                bounds_sent.append((copy, sends, receives))

    reach = near
    stage = 0
    if reach < count - 1:
        greet(ready.at[0], reach)

    lines = []
    for i in range(blocks):
        target = send_order(me, count, i)
        line = jnp.int32(0)
        for j in range(blocks):
            line = jnp.where(dest[j] // blocks == target, j, line)
        order[i] = line
        lines.append(line)
    c0 = column([az_coef[0, j] for j in lines])
    c1 = column([az_coef[1, j] for j in lines])
    c2 = column([az_coef[2, j] for j in lines])
    q = 0.5
    fraction = c0 + c1 * q + c2 * q * q
    band = azimuth_band(fraction, column([az_base[j] for j in lines]), column(lines), blocks)
    band = band[:, : blocks + 2 * HALO]
    range_weights(coef, start, weight, cols)
    while reach < count - 1:
        pl.semaphore_wait(
            ready.at[stage], (me >= reach).astype(jnp.int32) + (me + reach < count).astype(jnp.int32)
        )
        reach, stage = 2 * reach, stage + 1
        if reach < count - 1:
            greet(ready.at[stage], reach)

    for copy, sends, receives in bounds_sent:
        finish(copy, sends, receives)
    low = edge[0]
    high = edge[1]
    row = lax.broadcasted_iota(jnp.int32, high.shape, 0)
    outside = ((me == 0) & (row >= blocks) & (row < blocks + HALO)) | (
        (me == count - 1) & (row >= blocks + HALO)
    )
    high = jnp.where(outside, 0.0, high)
    lane_held = lax.broadcasted_iota(jnp.int32, high.shape, 1).astype(jnp.float32)
    lane_row = lax.broadcasted_iota(jnp.int32, (blocks, 128), 1)
    lane = lax.broadcasted_iota(jnp.int32, (8, 128), 1)

    def azimuth(first_tile, wide, tails):
        at = pl.ds(first_tile * 128, wide * 128)
        keeps = []
        for u in range(wide):
            col = lane_held + ((first_tile + u) * 128.0)
            keeps.append((col >= low) & (col < high))
        new_tails = []
        for p in range(2):
            rows = held[p, :, at].astype(jnp.float32)
            rows = jnp.concatenate(
                [
                    jnp.where(keep, rows[:, u * 128 : u * 128 + 128], 0.0)
                    for u, keep in enumerate(keeps)
                ],
                axis=1,
            ).astype(jnp.bfloat16)
            out = jnp.dot(band, rows, preferred_element_type=jnp.float32)
            out = out.astype(jnp.bfloat16).astype(jnp.float32)
            tail = tails[p]
            for u in range(wide):
                turned = pltpu.roll(out[:, u * 128 : u * 128 + 128], 64, 1)
                place = p * blocks * span + first_tile + u
                dense[pl.ds(place, blocks, stride=span), :] = jnp.where(lane_row < 64, tail, turned)
                tail = turned
            new_tails.append(tail)
        return tuple(new_tails)

    def filtered(i, big, power):
        for p in range(2):
            halves = []
            for h in range(2):
                g = big * 2 + h
                b = shift[order[i]] + start[g] + 64
                at = pl.multiple_of((p * blocks + i) * span + g * 8, 8)
                x0 = dense[pl.ds(at, 8), :]
                x1 = dense[pl.ds(at + 1, 8), :]
                acc = None
                for k in range(TAPS):
                    moved = pltpu.roll(jnp.where(lane < b + k, x1, x0), 128 - b - k, 1)
                    term = weight[g, k] * moved
                    acc = term if acc is None else acc + term
                halves.append(acc)
            done = jnp.concatenate(halves, axis=0).astype(jnp.bfloat16)
            sent[i, p, pl.ds(pl.multiple_of(big * 16, 16), 16), :] = done
            wide = done.astype(jnp.float32)
            power = power + wide * wide
        return power

    def parcel(c, i):
        at = pl.ds(cuts[c] * 16, (cuts[c + 1] - cuts[c]) * 16)
        peer = send_order(me, count, i)
        return pltpu.make_async_remote_copy(
            src_ref=sent.at[i, :, at, :],
            dst_ref=got.at[me, :, at, :],
            send_sem=send_sem.at[c, i],
            recv_sem=recv_sem.at[c, me],
            device_id={"az": peer},
        )

    tails = (jnp.zeros((blocks, 128), jnp.float32),) * 2
    power = jnp.zeros((16, 128), jnp.float32)
    for c in range(chunks):
        for copy, sends, receives in halo[2 * c : 2 * c + 2]:
            finish(copy, sends, receives)
        for first_tile in range(bounds[c], bounds[c + 1], WIDE):
            tails = azimuth(first_tile, min(WIDE, bounds[c + 1] - first_tile), tails)
        if c == chunks - 1:
            for p in range(2):
                ends = jnp.where(lane_row < 64, tails[p], 0.0)
                dense[pl.ds(p * blocks * span + tiles, blocks, stride=span), :] = ends
        lo, hi = cuts[c], cuts[c + 1]

        def line(i, power):
            power = lax.fori_loop(lo, hi, functools.partial(filtered, i), power, unroll=True)
            if c < chunks - 1:

                @pl.when(i < count - 1)
                def _():
                    parcel(c, i).start()

            return power

        power = lax.fori_loop(0, blocks, line, power)

    own_power = jnp.broadcast_to(jnp.sum(power, keepdims=True), (1, 128))
    have = jnp.int32(0)
    for j in range(blocks):
        have = have + jnp.maximum(
            jnp.minimum(high_edge[j], cols) - jnp.maximum(low_edge[j], 0), 0
        )
    own_count = jnp.full((1, 128), have, jnp.int32).astype(jnp.float32)
    lane_note = lax.broadcasted_iota(jnp.int32, (1, 128), 1)
    stats = jnp.where(lane_note == 127, own_power, own_count)
    for i in range(blocks):
        place = jnp.full((1, 128), dest[lines[i]] % blocks, jnp.int32).astype(jnp.float32)
        memo[i] = jnp.where(lane_note < 126, place, stats)

    def told(i):
        return pltpu.make_async_remote_copy(
            src_ref=memo.at[i],
            dst_ref=notes.at[me],
            send_sem=note_send.at[i],
            recv_sem=note_recv.at[me],
            device_id={"az": send_order(me, count, i)},
        )

    def tell(i, carry):
        told(i).start()
        return carry

    def last_send(i, carry):
        parcel(chunks - 1, i).start()
        return carry

    lax.fori_loop(0, count - 1, tell, 0)
    lax.fori_loop(0, count - 1, last_send, 0)
    notes[me] = memo[blocks - 1]
    got[me] = sent[blocks - 1]

    for c in range(chunks):
        lo, wide = cuts[c] * 16, (cuts[c + 1] - cuts[c]) * 16
        at = pl.ds(lo, wide)

        def take(i, carry):
            peer = send_order(me, count, i)
            parcel(c, i).wait_send()
            pltpu.make_async_remote_copy(
                src_ref=sent.at[i, :, at, :],
                dst_ref=got.at[peer, :, at, :],
                send_sem=send_sem.at[c, i],
                recv_sem=recv_sem.at[c, peer],
                device_id={"az": peer},
            ).wait_recv()
            return carry

        lax.fori_loop(0, count - 1, take, 0)

        def spread(s, carry):
            for p in range(2):
                dense[pl.ds((p * blocks + s) * span + lo, wide), :] = got[s, p, at, :].astype(jnp.float32)
            return carry

        lax.fori_loop(0, blocks, spread, 0)
        for t in range(lo, lo + wide):
            for p in range(2):
                x = dense[pl.ds(p * blocks * span + t, blocks, stride=span), :]
                nat[p, :, t * 128 : t * 128 + 128] = x.astype(jnp.bfloat16)

    def hear(i, carry):
        peer = send_order(me, count, i)
        told(i).wait_send()
        pltpu.make_async_remote_copy(
            src_ref=memo.at[i],
            dst_ref=notes.at[peer],
            send_sem=note_send.at[i],
            recv_sem=note_recv.at[peer],
            device_id={"az": peer},
        ).wait_recv()
        return carry

    lax.fori_loop(0, count - 1, hear, 0)


def finish_kernel(total, parts, nat, notes, out, mean, share, scaled, done):
    blocks, cols = out.shape[1], out.shape[2]
    told = [notes[s] for s in range(blocks)]
    both = functools.reduce(lambda a, b: a + b, told)
    power, count = both[:, 127:128], both[:, 126:127]
    mean_power = power / jnp.maximum(count, 1.0)
    gain = lax.rsqrt(mean_power + 0.5)
    lane = lax.broadcasted_iota(jnp.int32, (1, 128), 1)
    place = functools.reduce(
        lambda a, s: jnp.where(lane == s, told[s], a), range(blocks), jnp.full((1, 128), -1.0)
    )
    row = lax.broadcasted_iota(jnp.int32, (blocks, 128), 0).astype(jnp.float32)
    pick = (row == place).astype(jnp.float32).astype(jnp.bfloat16)[:, :blocks]
    copies = []
    piece = cols // parts
    for c in range(parts):
        for p in range(2):
            for t in range(c * piece, (c + 1) * piece, 1024):
                wide = min(1024, (c + 1) * piece - t)
                x = jnp.dot(pick, nat[p, :, t : t + wide], preferred_element_type=jnp.float32)
                scaled[p, :, t : t + wide] = (x * gain).astype(jnp.bfloat16)
            at = pl.ds(c * piece, piece)
            copy = pltpu.make_async_copy(
                scaled.at[p, :, at], out.at[p, :, at], done.at[2 * c + p]
            )
            copy.start()
            copies.append(copy)
    mean[0] = mean_power[0, 0]
    share[0] = (count / float(total))[0, 0]
    for copy in copies:
        copy.wait()


def shards(
    secondary, line_valid, first_valid, last_valid, az_coef, az_base, rg_base, rg_coef, block_dest
):
    cols = secondary.shape[2]
    blocks = block_dest.shape[0]
    tiles = cols // 128
    count = lax.axis_size("az")
    bigs = tiles // 16
    cuts = [0] + sorted({bigs * cut // 6 for cut in CUTS} - {0, bigs}) + [bigs]
    chunks = len(cuts) - 1
    parts = max(c for c in range(1, PARTS + 1) if bigs % c == 0)
    vmem = pl.BlockSpec(memory_space=pltpu.VMEM)
    smem = pl.BlockSpec(memory_space=pltpu.SMEM)
    held = blocks + 2 * HALO
    dma = pltpu.SemaphoreType.DMA
    stages = max(1, (-(-count // NEAR)).bit_length())
    nat, notes = pl.pallas_call(
        functools.partial(swath_kernel, cuts),
        out_shape=(
            pltpu.VMEM((2, blocks, cols), jnp.bfloat16),
            pltpu.VMEM((blocks, 1, 128), jnp.float32),
        ),
        in_specs=[pl.BlockSpec(memory_space=pl.ANY)] * 9,
        out_specs=(vmem, vmem),
        scratch_shapes=[
            pltpu.SMEM(rg_coef.shape, jnp.float32),
            pltpu.SMEM((blocks,), jnp.int32),
            pltpu.SMEM((blocks,), jnp.int32),
            pltpu.SMEM((blocks,), jnp.int32),
            pltpu.SMEM((blocks,), jnp.int32),
            pltpu.SMEM((blocks,), jnp.int32),
            pltpu.SMEM(az_coef.shape, jnp.float32),
            pltpu.SMEM((blocks,), jnp.int32),
            pltpu.VMEM((2, held, cols), jnp.bfloat16),
            pltpu.VMEM((2, held, 128), jnp.float32),
            pltpu.VMEM((2 * blocks * (tiles + 8), 128), jnp.float32),
            pltpu.VMEM((tiles // 8, TAPS, 8, 128), jnp.float32),
            pltpu.VMEM((blocks, 2, tiles, 128), jnp.bfloat16),
            pltpu.VMEM((blocks, 2, tiles, 128), jnp.bfloat16),
            pltpu.VMEM((blocks, 1, 128), jnp.float32),
            pltpu.SMEM((tiles // 8,), jnp.int32),
            pltpu.SMEM((blocks,), jnp.int32),
            pltpu.SemaphoreType.REGULAR((stages,)),
            dma((8,)),
            dma(()),
            dma((chunks, 2)),
            dma((chunks, 2)),
            dma((2,)),
            dma((2,)),
            dma((chunks, blocks)),
            dma((chunks, blocks)),
            dma((blocks,)),
            dma((blocks,)),
        ],
        compiler_params=pltpu.CompilerParams(collective_id=0, has_side_effects=True),
        name="swath",
    )(
        rg_coef, rg_base, block_dest, line_valid, first_valid, last_valid, az_coef, az_base,
        secondary,
    )
    return pl.pallas_call(
        functools.partial(finish_kernel, cols * blocks * count, parts),
        out_shape=(
            jax.ShapeDtypeStruct((2, blocks, cols), jnp.bfloat16),
            jax.ShapeDtypeStruct((1,), jnp.float32),
            jax.ShapeDtypeStruct((1,), jnp.float32),
        ),
        in_specs=[vmem, vmem],
        out_specs=(pl.BlockSpec(memory_space=pl.ANY), smem, smem),
        scratch_shapes=[pltpu.VMEM((2, blocks, cols), jnp.bfloat16), dma((2 * parts,))],
        name="finish",
    )(
        pltpu.with_memory_space_constraint(nat, pltpu.VMEM),
        pltpu.with_memory_space_constraint(notes, pltpu.VMEM),
    )


CUTS = (1, 3)
PARTS = 2
NEAR = 4
WIDE = 9


def solution(mesh):
    rows = P(("scene", "az"))
    placed = (
        P(None, ("scene", "az"), None),
        rows,
        rows,
        rows,
        P(None, ("scene", "az")),
        rows,
        rows,
        P("scene"),
        rows,
    )
    return jax.shard_map(
        shards,
        mesh=mesh,
        in_specs=placed,
        out_specs=(P(None, ("scene", "az"), None), P("scene"), P("scene")),
        check_vma=False,
    )
```

```python
import functools
import math

import jax
import jax.numpy as jnp
from jax import lax
from jax.experimental import pallas as pl
from jax.experimental.pallas import tpu as pltpu
from jax.sharding import PartitionSpec as P

HALO = 8
GROUP = 2048
RANGE_LIMIT = 3.0
NOTE = 8
PI = 3.141592653589793
HALF = 0.7071067811865476
COS8 = (1.0, HALF, 0.0, -HALF, -1.0, -HALF, 0.0, HALF)


def range_spread(cols):
    half = GROUP / 2 / cols
    return RANGE_LIMIT * (half + 1.0 - (1.0 - half) ** 2 + 1.0 - (1.0 - half) ** 3) + 0.03


def range_taps(cols):
    return math.ceil(2.0 * (4.0 + range_spread(cols)))


def range_weights(coef, start, weight, cols):
    reach = 4.0 + range_spread(cols)
    for g in range(cols // GROUP):
        centre = (g + 0.5) * GROUP / cols
        oc = coef[0] + coef[1] * centre + coef[2] * (centre * centre) + coef[3] * (centre**3)
        n0 = (oc - reach + 64.0).astype(jnp.int32) - 63
        start[g] = n0
        sub = lax.broadcasted_iota(jnp.int32, (GROUP // 128, 128), 0)
        lane = lax.broadcasted_iota(jnp.int32, (GROUP // 128, 128), 1)
        col = g * GROUP + sub * 128 + lane
        v = (col.astype(jnp.float32) + 0.5) / cols
        off = coef[0] + coef[1] * v + coef[2] * v * v + coef[3] * v * v * v
        whole = jnp.round(off)
        part = off - whole
        odd = (whole.astype(jnp.int32) + n0) & 1
        sine = jnp.sin(PI * part) * (-1.0 / PI) * (1 - 2 * odd).astype(jnp.float32)
        base = (n0.astype(jnp.float32) - off) * (PI / 4.0)
        c0, s0 = jnp.cos(base), jnp.sin(base)
        for k in range(weight.shape[1]):
            n = n0 + k
            d = n.astype(jnp.float32) - off
            ck, sk = COS8[k % 8], COS8[(k - 2) % 8]
            taper = 0.5 + 0.5 * (c0 * ck - s0 * sk)
            top = sine if k % 2 == 0 else -sine
            near = d == 0.0
            val = jnp.where(near, 1.0, top / jnp.where(near, 1.0, d)) * taper
            keep = (jnp.abs(d) < 4.0) & (col + n >= 0) & (col + n < cols)
            val = jnp.where(keep, val, 0.0)
            weight[g, k] = val.astype(jnp.bfloat16).astype(jnp.float32)


def column(values):
    row = lax.broadcasted_iota(jnp.int32, (len(values), 128), 0)
    made = jnp.zeros((len(values), 128), jnp.asarray(values[0]).dtype)
    for r, value in enumerate(values):
        made = jnp.where(row == r, value, made)
    return made


def azimuth_band(fraction, base, line, blocks):
    held = lax.broadcasted_iota(jnp.int32, (blocks, 128), 1)
    row = jnp.where(held < blocks, held, held - blocks - HALO)
    row = jnp.where(held < blocks + HALO, row, held - HALO)
    gap = row - line - base
    d = gap.astype(jnp.float32) - fraction
    near = d == 0.0
    safe = jnp.where(near, 1.0, d)
    whole = jnp.round(safe)
    sine = jnp.sin(PI * (safe - whole)) * (1 - 2 * (whole.astype(jnp.int32) & 1)).astype(jnp.float32)
    value = jnp.where(near, 1.0, sine / (PI * safe)) * (0.5 + 0.5 * jnp.cos(PI * d / 4.0))
    keep = (jnp.abs(d) < 4.0) & (jnp.abs(gap) <= 4) & (held < blocks + 2 * HALO)
    return jnp.where(keep, value, 0.0).astype(jnp.bfloat16)


def send_order(me, count, i):
    half = count // 2
    mine = me // half
    own = i // half
    side = mine * own + (1 - mine) * (1 - own)
    near = lax.rem(me - mine * half + own + i - own * half, half)
    if half % 2:
        return side * half + near
    quarter = half // 2
    group = i // quarter
    far = (mine * group + (1 - mine) * (1 - group)) * quarter + lax.rem(me + i, quarter)
    return side * half + jnp.where(own == 1, near, far)


def swath_kernel(
    cuts, coef_in, shift_in, dest_in, valid_in, first_in, last_in, az_coef_in, az_base_in, image,
    nat, notes,
    coef, shift, dest, valid, first, last, az_coef, az_base,
    held, edge, dense, weight, sent, got, memo, start, order,
    ready, load_sem, own_sem, halo_send, halo_recv, edge_send, edge_recv, send_sem, recv_sem, note_send, note_recv,
):
    blocks, cols = image.shape[1], image.shape[2]
    tiles = cols // 128
    span = dense.shape[0] // (2 * blocks)
    count = lax.axis_size("az")
    me = lax.axis_index("az")
    after, before = lax.rem(me + 1, count), lax.rem(me + count - 1, count)
    up, down = me < count - 1, me > 0

    barrier = pltpu.get_barrier_semaphore()
    near = min(NEAR, count - 1)

    def greet(semaphore, step):
        @pl.when(me + step < count)
        def _():
            pl.semaphore_signal(semaphore, inc=1, device_id={"az": lax.rem(me + step, count)})

        @pl.when(me >= step)
        def _():
            pl.semaphore_signal(semaphore, inc=1, device_id={"az": lax.rem(me + count - step, count)})

    for step in range(1, near + 1):
        greet(barrier, step)
    own = pltpu.make_async_copy(image, held.at[:, pl.ds(0, blocks)], own_sem)
    own.start()
    loads = [
        pltpu.make_async_copy(source, target, load_sem.at[k])
        for k, (source, target) in enumerate(
            (
                (valid_in, valid), (first_in, first), (last_in, last), (coef_in, coef),
                (shift_in, shift), (dest_in, dest), (az_coef_in, az_coef), (az_base_in, az_base),
            )
        )
    ]
    for load in loads:
        load.start()
    for load in loads:
        load.wait()
    low_edge = [jnp.where(valid[r] > 0, first[r], cols) for r in range(blocks)]
    high_edge = [jnp.where(valid[r] > 0, last[r], 0) for r in range(blocks)]
    edge[0, pl.ds(0, blocks), :] = column(low_edge).astype(jnp.float32)
    edge[1, pl.ds(0, blocks), :] = column(high_edge).astype(jnp.float32)
    own.wait()
    pl.semaphore_wait(barrier, jnp.minimum(me, near) + jnp.minimum(count - 1 - me, near))

    chunks = len(cuts) - 1
    bounds = [0] + [cut * 16 + 1 for cut in cuts[1:-1]] + [tiles]
    ways = ((after, blocks - HALO, blocks, up, down), (before, 0, blocks + HALO, down, up))

    def begin(copy, sends):
        @pl.when(sends)
        def _():
            copy.start()

    def finish(copy, sends, receives):
        @pl.when(sends)
        def _():
            copy.wait_send()

        @pl.when(receives)
        def _():
            copy.wait_recv()

    halo = []
    for c in range(chunks):
        at = pl.ds(bounds[c] * 128, (bounds[c + 1] - bounds[c]) * 128)
        for w, (peer, source, slot, sends, receives) in enumerate(ways):
            copy = pltpu.make_async_remote_copy(
                src_ref=held.at[:, pl.ds(source, HALO), at],
                dst_ref=held.at[:, pl.ds(slot, HALO), at],
                send_sem=halo_send.at[c, w],
                recv_sem=halo_recv.at[c, w],
                device_id={"az": peer},
            )
            begin(copy, sends)
            halo.append((copy, sends, receives))
        if c == 0:
            bounds_sent = []
            for w, (peer, source, slot, sends, receives) in enumerate(ways):
                copy = pltpu.make_async_remote_copy(
                    src_ref=edge.at[:, pl.ds(source, HALO), :],
                    dst_ref=edge.at[:, pl.ds(slot, HALO), :],
                    send_sem=edge_send.at[w],
                    recv_sem=edge_recv.at[w],
                    device_id={"az": peer},
                )
                begin(copy, sends)
                bounds_sent.append((copy, sends, receives))

    reach = near
    stage = 0
    if reach < count - 1:
        greet(ready.at[0], reach)

    lines = []
    for i in range(blocks):
        target = send_order(me, count, i)
        line = jnp.int32(0)
        for j in range(blocks):
            line = jnp.where(dest[j] // blocks == target, j, line)
        order[i] = line
        lines.append(line)
    c0 = column([az_coef[0, j] for j in lines])
    c1 = column([az_coef[1, j] for j in lines])
    c2 = column([az_coef[2, j] for j in lines])
    q = 0.5
    fraction = c0 + c1 * q + c2 * q * q
    band = azimuth_band(fraction, column([az_base[j] for j in lines]), column(lines), blocks)
    band = band[:, : blocks + 2 * HALO]
    range_weights(coef, start, weight, cols)
    while reach < count - 1:
        pl.semaphore_wait(
            ready.at[stage], (me >= reach).astype(jnp.int32) + (me + reach < count).astype(jnp.int32)
        )
        reach, stage = 2 * reach, stage + 1
        if reach < count - 1:
            greet(ready.at[stage], reach)

    for copy, sends, receives in bounds_sent:
        finish(copy, sends, receives)
    low = edge[0]
    high = edge[1]
    row = lax.broadcasted_iota(jnp.int32, high.shape, 0)
    outside = ((me == 0) & (row >= blocks) & (row < blocks + HALO)) | (
        (me == count - 1) & (row >= blocks + HALO)
    )
    high = jnp.where(outside, 0.0, high)
    lane_held = lax.broadcasted_iota(jnp.int32, high.shape, 1).astype(jnp.float32)
    lane_row = lax.broadcasted_iota(jnp.int32, (blocks, 128), 1)
    lane = lax.broadcasted_iota(jnp.int32, (16, 128), 1)

    def azimuth(first_tile, wide, tails):
        at = pl.ds(first_tile * 128, wide * 128)
        keeps = []
        for u in range(wide):
            col = lane_held + ((first_tile + u) * 128.0)
            keeps.append((col >= low) & (col < high))
        new_tails = []
        for p in range(2):
            rows = held[p, :, at].astype(jnp.float32)
            rows = jnp.concatenate(
                [
                    jnp.where(keep, rows[:, u * 128 : u * 128 + 128], 0.0)
                    for u, keep in enumerate(keeps)
                ],
                axis=1,
            ).astype(jnp.bfloat16)
            out = jnp.dot(band, rows, preferred_element_type=jnp.float32)
            out = out.astype(jnp.bfloat16).astype(jnp.float32)
            tail = tails[p]
            for u in range(wide):
                turned = pltpu.roll(out[:, u * 128 : u * 128 + 128], 64, 1)
                place = p * blocks * span + first_tile + u
                dense[pl.ds(place, blocks, stride=span), :] = jnp.where(lane_row < 64, tail, turned)
                tail = turned
            new_tails.append(tail)
        return tuple(new_tails)

    def filtered(i, big, power):
        b = shift[order[i]] + start[big] + 64
        for p in range(2):
            at = pl.multiple_of((p * blocks + i) * span + big * 16, 8)
            x0 = dense[pl.ds(at, 16), :]
            x1 = dense[pl.ds(at + 1, 16), :]
            acc = None
            for k in range(weight.shape[1]):
                moved = pltpu.roll(jnp.where(lane < b + k, x1, x0).astype(jnp.bfloat16), 128 - b - k, 1)
                term = weight[big, k] * moved.astype(jnp.float32)
                acc = term if acc is None else acc + term
            done = acc.astype(jnp.bfloat16)
            sent[i, p, pl.ds(pl.multiple_of(big * 16, 16), 16), :] = done
            wide = done.astype(jnp.float32)
            power = power + wide * wide
        return power

    def parcel(c, i):
        at = pl.ds(cuts[c] * 16, (cuts[c + 1] - cuts[c]) * 16)
        peer = send_order(me, count, i)
        return pltpu.make_async_remote_copy(
            src_ref=sent.at[i, :, at, :],
            dst_ref=got.at[me, :, at, :],
            send_sem=send_sem.at[c, i],
            recv_sem=recv_sem.at[c, me],
            device_id={"az": peer},
        )

    tails = (jnp.zeros((blocks, 128), jnp.float32),) * 2
    power = jnp.zeros((16, 128), jnp.float32)
    half = count // 2
    far, near_half, own_half = (0, half // 2), (half // 2, half), (half, blocks)

    def post(c, lines_at):
        def body(i, carry):
            parcel(c, i).start()
            return carry

        lax.fori_loop(lines_at[0], min(lines_at[1], count - 1), body, 0)

    def lines_of(c, lines_at, power, send):
        def line(i, power):
            power = lax.fori_loop(
                cuts[c], cuts[c + 1], functools.partial(filtered, i), power, unroll=True
            )
            if send:

                @pl.when(i < count - 1)
                def _():
                    parcel(c, i).start()

            return power

        return lax.fori_loop(*lines_at, line, power)

    for c in range(chunks):
        for copy, sends, receives in halo[2 * c : 2 * c + 2]:
            finish(copy, sends, receives)
        for first_tile in range(bounds[c], bounds[c + 1], WIDE):
            tails = azimuth(first_tile, min(WIDE, bounds[c + 1] - first_tile), tails)
        if c == chunks - 1:
            for p in range(2):
                ends = jnp.where(lane_row < 64, tails[p], 0.0)
                dense[pl.ds(p * blocks * span + tiles, blocks, stride=span), :] = ends
        power = lines_of(c, far, power, True)
        if c < chunks - 1:
            power = lines_of(*((0, near_half) if c == 0 else (c - 1, own_half)), power, True)
    for c in range(1, chunks - 1):
        power = lines_of(c, near_half, power, True)
    power = lines_of(chunks - 1, near_half, power, False)
    late = [c for c in (chunks - 2, chunks - 1) if c >= 0]
    for c in late:
        power = lines_of(c, own_half, power, False)

    own_power = jnp.broadcast_to(jnp.sum(power, keepdims=True), (1, 128))
    have = jnp.int32(0)
    for j in range(blocks):
        have = have + jnp.maximum(
            jnp.minimum(high_edge[j], cols) - jnp.maximum(low_edge[j], 0), 0
        )
    own_count = jnp.full((1, 128), have, jnp.int32).astype(jnp.float32)
    lane_note = lax.broadcasted_iota(jnp.int32, (1, 128), 1)
    stats = jnp.where(lane_note == 127, own_power, own_count)
    for i in range(blocks):
        place = jnp.full((1, 128), dest[lines[i]] % blocks, jnp.int32).astype(jnp.float32)
        memo[i] = jnp.where(lane_note < 126, place, stats)

    def told(i):
        return pltpu.make_async_remote_copy(
            src_ref=memo.at[i],
            dst_ref=notes.at[me],
            send_sem=note_send.at[i],
            recv_sem=note_recv.at[me],
            device_id={"az": send_order(me, count, i)},
        )

    def tell(i, carry):
        told(i).start()
        return carry

    lax.fori_loop(0, count - 1, tell, 0)
    post(chunks - 1, near_half)
    for c in late:
        post(c, own_half)
    notes[me] = memo[blocks - 1]
    got[me] = sent[blocks - 1]

    for c in range(chunks):
        lo, wide = cuts[c] * 16, (cuts[c + 1] - cuts[c]) * 16
        at = pl.ds(lo, wide)

        def take(i, carry):
            peer = send_order(me, count, i)
            parcel(c, i).wait_send()
            pltpu.make_async_remote_copy(
                src_ref=sent.at[i, :, at, :],
                dst_ref=got.at[peer, :, at, :],
                send_sem=send_sem.at[c, i],
                recv_sem=recv_sem.at[c, peer],
                device_id={"az": peer},
            ).wait_recv()
            return carry

        lax.fori_loop(0, count - 1, take, 0)

        def spread(s, carry):
            for p in range(2):
                dense[pl.ds((p * blocks + s) * span + lo, wide), :] = got[s, p, at, :].astype(jnp.float32)
            return carry

        lax.fori_loop(0, blocks, spread, 0)
        for t in range(lo, lo + wide):
            for p in range(2):
                x = dense[pl.ds(p * blocks * span + t, blocks, stride=span), :]
                nat[p, :, t * 128 : t * 128 + 128] = x.astype(jnp.bfloat16)

    def hear(i, carry):
        peer = send_order(me, count, i)
        told(i).wait_send()
        pltpu.make_async_remote_copy(
            src_ref=memo.at[i],
            dst_ref=notes.at[peer],
            send_sem=note_send.at[i],
            recv_sem=note_recv.at[peer],
            device_id={"az": peer},
        ).wait_recv()
        return carry

    lax.fori_loop(0, count - 1, hear, 0)


def finish_kernel(total, parts, nat, notes, out, mean, share, scaled, figures, done):
    blocks, cols = out.shape[1], out.shape[2]
    told = [notes[s] for s in range(blocks)]
    both = functools.reduce(lambda a, b: a + b, told)
    power, count = both[:, 127:128], both[:, 126:127]
    mean_power = power / jnp.maximum(count, 1.0)
    gain = lax.rsqrt(mean_power + 0.5)
    lane = lax.broadcasted_iota(jnp.int32, (1, 128), 1)
    place = functools.reduce(
        lambda a, s: jnp.where(lane == s, told[s], a), range(blocks), jnp.full((1, 128), -1.0)
    )
    row = lax.broadcasted_iota(jnp.int32, (blocks, 128), 0).astype(jnp.float32)
    pick = (row == place).astype(jnp.float32).astype(jnp.bfloat16)[:, :blocks]
    figures[0, 0] = mean_power[0, 0]
    figures[1, 0] = (count / float(total))[0, 0]
    copies = [
        pltpu.make_async_copy(figures.at[k], target, done.at[k]) for k, target in enumerate((mean, share))
    ]
    for copy in copies:
        copy.start()
    piece = cols // parts
    for c in range(parts):
        for p in range(2):
            for t in range(c * piece, (c + 1) * piece, 1024):
                wide = min(1024, (c + 1) * piece - t)
                x = jnp.dot(pick, nat[p, :, t : t + wide], preferred_element_type=jnp.float32)
                scaled[p, :, t : t + wide] = (x * gain).astype(jnp.bfloat16)
            at = pl.ds(c * piece, piece)
            copy = pltpu.make_async_copy(
                scaled.at[p, :, at], out.at[p, :, at], done.at[2 + 2 * c + p]
            )
            copy.start()
            copies.append(copy)
    for copy in copies:
        copy.wait()


def shards(
    secondary, line_valid, first_valid, last_valid, az_coef, az_base, rg_base, rg_coef, block_dest
):
    cols = secondary.shape[2]
    blocks = block_dest.shape[0]
    tiles = cols // 128
    count = lax.axis_size("az")
    bigs = tiles // 16
    cuts = [0] + sorted({bigs * cut // 6 for cut in CUTS} - {0, bigs}) + [bigs]
    chunks = len(cuts) - 1
    parts = max(c for c in range(1, PARTS + 1) if bigs % c == 0)
    vmem = pl.BlockSpec(memory_space=pltpu.VMEM)
    held = blocks + 2 * HALO
    dma = pltpu.SemaphoreType.DMA
    stages = max(1, (-(-count // NEAR)).bit_length())
    nat, notes = pl.pallas_call(
        functools.partial(swath_kernel, cuts),
        out_shape=(
            pltpu.VMEM((2, blocks, cols), jnp.bfloat16),
            pltpu.VMEM((blocks, 1, 128), jnp.float32),
        ),
        in_specs=[pl.BlockSpec(memory_space=pl.ANY)] * 9,
        out_specs=(vmem, vmem),
        scratch_shapes=[
            pltpu.SMEM(rg_coef.shape, jnp.float32),
            pltpu.SMEM((blocks,), jnp.int32),
            pltpu.SMEM((blocks,), jnp.int32),
            pltpu.SMEM((blocks,), jnp.int32),
            pltpu.SMEM((blocks,), jnp.int32),
            pltpu.SMEM((blocks,), jnp.int32),
            pltpu.SMEM(az_coef.shape, jnp.float32),
            pltpu.SMEM((blocks,), jnp.int32),
            pltpu.VMEM((2, held, cols), jnp.bfloat16),
            pltpu.VMEM((2, held, 128), jnp.float32),
            pltpu.VMEM((2 * blocks * (tiles + 8), 128), jnp.float32),
            pltpu.VMEM((cols // GROUP, range_taps(cols), GROUP // 128, 128), jnp.float32),
            pltpu.VMEM((blocks, 2, tiles, 128), jnp.bfloat16),
            pltpu.VMEM((blocks, 2, tiles, 128), jnp.bfloat16),
            pltpu.VMEM((blocks, 1, 128), jnp.float32),
            pltpu.SMEM((cols // GROUP,), jnp.int32),
            pltpu.SMEM((blocks,), jnp.int32),
            pltpu.SemaphoreType.REGULAR((stages,)),
            dma((8,)),
            dma(()),
            dma((chunks, 2)),
            dma((chunks, 2)),
            dma((2,)),
            dma((2,)),
            dma((chunks, blocks)),
            dma((chunks, blocks)),
            dma((blocks,)),
            dma((blocks,)),
        ],
        compiler_params=pltpu.CompilerParams(collective_id=0, has_side_effects=True),
        name="swath",
    )(
        rg_coef, rg_base, block_dest, line_valid, first_valid, last_valid, az_coef, az_base,
        secondary,
    )
    return pl.pallas_call(
        functools.partial(finish_kernel, cols * blocks * count, parts),
        out_shape=(
            jax.ShapeDtypeStruct((2, blocks, cols), jnp.bfloat16),
            jax.ShapeDtypeStruct((1,), jnp.float32),
            jax.ShapeDtypeStruct((1,), jnp.float32),
        ),
        in_specs=[vmem, vmem],
        out_specs=(pl.BlockSpec(memory_space=pl.ANY),) * 3,
        scratch_shapes=[
            pltpu.VMEM((2, blocks, cols), jnp.bfloat16),
            pltpu.SMEM((2, 1), jnp.float32),
            dma((2 + 2 * parts,)),
        ],
        name="finish",
    )(
        pltpu.with_memory_space_constraint(nat, pltpu.VMEM),
        pltpu.with_memory_space_constraint(notes, pltpu.VMEM),
    )


CUTS = (1, 3)
PARTS = 2
NEAR = 4
WIDE = 9


def solution(mesh):
    rows = P(("scene", "az"))
    placed = (
        P(None, ("scene", "az"), None),
        rows,
        rows,
        rows,
        P(None, ("scene", "az")),
        rows,
        rows,
        P("scene"),
        rows,
    )
    return jax.shard_map(
        shards,
        mesh=mesh,
        in_specs=placed,
        out_specs=(P(None, ("scene", "az"), None), P("scene"), P("scene")),
        check_vma=False,
    )
```

```python
import functools
import math

import jax
import jax.numpy as jnp
from jax import lax
from jax.experimental import pallas as pl
from jax.experimental.pallas import tpu as pltpu
from jax.sharding import PartitionSpec as P

HALO = 8
GROUP = 2048
RANGE_LIMIT = 3.0
NOTE = 8
PI = 3.141592653589793
HALF = 0.7071067811865476
COS8 = (1.0, HALF, 0.0, -HALF, -1.0, -HALF, 0.0, HALF)


def range_spread(cols):
    half = GROUP / 2 / cols
    return RANGE_LIMIT * (half + 1.0 - (1.0 - half) ** 2 + 1.0 - (1.0 - half) ** 3) + 0.03


def range_taps(cols):
    return math.ceil(2.0 * (4.0 + range_spread(cols)))


def range_weights(coef, start, weight, cols):
    reach = 4.0 + range_spread(cols)
    for g in range(cols // GROUP):
        centre = (g + 0.5) * GROUP / cols
        oc = coef[0] + coef[1] * centre + coef[2] * (centre * centre) + coef[3] * (centre**3)
        n0 = (oc - reach + 64.0).astype(jnp.int32) - 63
        start[g] = n0
        sub = lax.broadcasted_iota(jnp.int32, (GROUP // 128, 128), 0)
        lane = lax.broadcasted_iota(jnp.int32, (GROUP // 128, 128), 1)
        col = g * GROUP + sub * 128 + lane
        v = (col.astype(jnp.float32) + 0.5) / cols
        off = coef[0] + coef[1] * v + coef[2] * v * v + coef[3] * v * v * v
        whole = jnp.round(off)
        part = off - whole
        odd = (whole.astype(jnp.int32) + n0) & 1
        sine = jnp.sin(PI * part) * (-1.0 / PI) * (1 - 2 * odd).astype(jnp.float32)
        base = (n0.astype(jnp.float32) - off) * (PI / 4.0)
        c0, s0 = jnp.cos(base), jnp.sin(base)
        for k in range(weight.shape[1]):
            n = n0 + k
            d = n.astype(jnp.float32) - off
            ck, sk = COS8[k % 8], COS8[(k - 2) % 8]
            taper = 0.5 + 0.5 * (c0 * ck - s0 * sk)
            top = sine if k % 2 == 0 else -sine
            near = d == 0.0
            val = jnp.where(near, 1.0, top / jnp.where(near, 1.0, d)) * taper
            keep = (jnp.abs(d) < 4.0) & (col + n >= 0) & (col + n < cols)
            val = jnp.where(keep, val, 0.0)
            weight[g, k] = val.astype(jnp.bfloat16).astype(jnp.float32)


def column(values):
    row = lax.broadcasted_iota(jnp.int32, (len(values), 128), 0)
    made = jnp.zeros((len(values), 128), jnp.asarray(values[0]).dtype)
    for r, value in enumerate(values):
        made = jnp.where(row == r, value, made)
    return made


def azimuth_band(fraction, base, line, blocks):
    held = lax.broadcasted_iota(jnp.int32, (blocks, 128), 1)
    row = jnp.where(held < blocks, held, held - blocks - HALO)
    row = jnp.where(held < blocks + HALO, row, held - HALO)
    gap = row - line - base
    d = gap.astype(jnp.float32) - fraction
    near = d == 0.0
    safe = jnp.where(near, 1.0, d)
    whole = jnp.round(safe)
    sine = jnp.sin(PI * (safe - whole)) * (1 - 2 * (whole.astype(jnp.int32) & 1)).astype(jnp.float32)
    value = jnp.where(near, 1.0, sine / (PI * safe)) * (0.5 + 0.5 * jnp.cos(PI * d / 4.0))
    keep = (jnp.abs(d) < 4.0) & (jnp.abs(gap) <= 4) & (held < blocks + 2 * HALO)
    return jnp.where(keep, value, 0.0).astype(jnp.bfloat16)


def send_order(me, count, i):
    half = count // 2
    mine = me // half
    own = i // half
    side = mine * own + (1 - mine) * (1 - own)
    near = lax.rem(me - mine * half + own + i - own * half, half)
    if half % 2:
        return side * half + near
    quarter = half // 2
    group = i // quarter
    far = (mine * group + (1 - mine) * (1 - group)) * quarter + lax.rem(me + i, quarter)
    return side * half + jnp.where(own == 1, near, far)


def swath_kernel(
    cuts, coef_in, shift_in, dest_in, valid_in, first_in, last_in, az_coef_in, az_base_in, image,
    nat, notes,
    coef, shift, dest, valid, first, last, az_coef, az_base,
    held, edge, dense, weight, sent, got, memo, start, order,
    ready, load_sem, own_sem, halo_send, halo_recv, edge_send, edge_recv, send_sem, recv_sem, note_send, note_recv,
):
    blocks, cols = image.shape[1], image.shape[2]
    tiles = cols // 128
    span = dense.shape[0] // (2 * blocks)
    count = lax.axis_size("az")
    me = lax.axis_index("az")
    after, before = lax.rem(me + 1, count), lax.rem(me + count - 1, count)
    up, down = me < count - 1, me > 0

    barrier = pltpu.get_barrier_semaphore()
    near = min(NEAR, count - 1)

    def greet(semaphore, step):
        @pl.when(me + step < count)
        def _():
            pl.semaphore_signal(semaphore, inc=1, device_id={"az": lax.rem(me + step, count)})

        @pl.when(me >= step)
        def _():
            pl.semaphore_signal(semaphore, inc=1, device_id={"az": lax.rem(me + count - step, count)})

    for step in range(1, near + 1):
        greet(barrier, step)
    own = pltpu.make_async_copy(image, held.at[:, pl.ds(0, blocks)], own_sem)
    own.start()
    loads = [
        pltpu.make_async_copy(source, target, load_sem.at[k])
        for k, (source, target) in enumerate(
            (
                (valid_in, valid), (first_in, first), (last_in, last), (coef_in, coef),
                (shift_in, shift), (dest_in, dest), (az_coef_in, az_coef), (az_base_in, az_base),
            )
        )
    ]
    for load in loads:
        load.start()
    for load in loads:
        load.wait()
    low_edge = [jnp.where(valid[r] > 0, first[r], cols) for r in range(blocks)]
    high_edge = [jnp.where(valid[r] > 0, last[r], 0) for r in range(blocks)]
    edge[0, pl.ds(0, blocks), :] = column(low_edge).astype(jnp.float32)
    edge[1, pl.ds(0, blocks), :] = column(high_edge).astype(jnp.float32)
    own.wait()
    pl.semaphore_wait(barrier, jnp.minimum(me, near) + jnp.minimum(count - 1 - me, near))

    chunks = len(cuts) - 1
    bounds = [0] + [cut * 16 + 1 for cut in cuts[1:-1]] + [tiles]
    ways = ((after, blocks - HALO, blocks, up, down), (before, 0, blocks + HALO, down, up))

    def begin(copy, sends):
        @pl.when(sends)
        def _():
            copy.start()

    def finish(copy, sends, receives):
        @pl.when(sends)
        def _():
            copy.wait_send()

        @pl.when(receives)
        def _():
            copy.wait_recv()

    halo = []
    for c in range(chunks):
        at = pl.ds(bounds[c] * 128, (bounds[c + 1] - bounds[c]) * 128)
        for w, (peer, source, slot, sends, receives) in enumerate(ways):
            copy = pltpu.make_async_remote_copy(
                src_ref=held.at[:, pl.ds(source, HALO), at],
                dst_ref=held.at[:, pl.ds(slot, HALO), at],
                send_sem=halo_send.at[c, w],
                recv_sem=halo_recv.at[c, w],
                device_id={"az": peer},
            )
            begin(copy, sends)
            halo.append((copy, sends, receives))
        if c == 0:
            bounds_sent = []
            for w, (peer, source, slot, sends, receives) in enumerate(ways):
                copy = pltpu.make_async_remote_copy(
                    src_ref=edge.at[:, pl.ds(source, HALO), :],
                    dst_ref=edge.at[:, pl.ds(slot, HALO), :],
                    send_sem=edge_send.at[w],
                    recv_sem=edge_recv.at[w],
                    device_id={"az": peer},
                )
                begin(copy, sends)
                bounds_sent.append((copy, sends, receives))

    reach = near
    stage = 0
    if reach < count - 1:
        greet(ready.at[0], reach)

    lines = []
    for i in range(blocks):
        target = send_order(me, count, i)
        line = jnp.int32(0)
        for j in range(blocks):
            line = jnp.where(dest[j] // blocks == target, j, line)
        order[i] = line
        lines.append(line)
    c0 = column([az_coef[0, j] for j in lines])
    c1 = column([az_coef[1, j] for j in lines])
    c2 = column([az_coef[2, j] for j in lines])
    q = 0.5
    fraction = c0 + c1 * q + c2 * q * q
    band = azimuth_band(fraction, column([az_base[j] for j in lines]), column(lines), blocks)
    band = band[:, : blocks + 2 * HALO]
    range_weights(coef, start, weight, cols)
    while reach < count - 1:
        pl.semaphore_wait(
            ready.at[stage], (me >= reach).astype(jnp.int32) + (me + reach < count).astype(jnp.int32)
        )
        reach, stage = 2 * reach, stage + 1
        if reach < count - 1:
            greet(ready.at[stage], reach)

    for copy, sends, receives in bounds_sent:
        finish(copy, sends, receives)
    low = edge[0]
    high = edge[1]
    row = lax.broadcasted_iota(jnp.int32, high.shape, 0)
    outside = ((me == 0) & (row >= blocks) & (row < blocks + HALO)) | (
        (me == count - 1) & (row >= blocks + HALO)
    )
    high = jnp.where(outside, 0.0, high)
    lane_held = lax.broadcasted_iota(jnp.int32, high.shape, 1).astype(jnp.float32)
    lane_row = lax.broadcasted_iota(jnp.int32, (blocks, 128), 1)
    lane = lax.broadcasted_iota(jnp.int32, (16, 128), 1)

    def azimuth(first_tile, wide, tails):
        at = pl.ds(first_tile * 128, wide * 128)
        keeps = []
        for u in range(wide):
            col = lane_held + ((first_tile + u) * 128.0)
            keeps.append((col >= low) & (col < high))
        new_tails = []
        for p in range(2):
            rows = held[p, :, at].astype(jnp.float32)
            rows = jnp.concatenate(
                [
                    jnp.where(keep, rows[:, u * 128 : u * 128 + 128], 0.0)
                    for u, keep in enumerate(keeps)
                ],
                axis=1,
            ).astype(jnp.bfloat16)
            out = jnp.dot(band, rows, preferred_element_type=jnp.float32)
            out = out.astype(jnp.bfloat16).astype(jnp.float32)
            tail = tails[p]
            for u in range(wide):
                turned = pltpu.roll(out[:, u * 128 : u * 128 + 128], 64, 1)
                place = p * blocks * span + first_tile + u
                dense[pl.ds(place, blocks, stride=span), :] = jnp.where(lane_row < 64, tail, turned)
                tail = turned
            new_tails.append(tail)
        return tuple(new_tails)

    def filtered(i, big, power):
        b = shift[order[i]] + start[big] + 64
        for p in range(2):
            at = pl.multiple_of((p * blocks + i) * span + big * 16, 8)
            x0 = dense[pl.ds(at, 16), :]
            x1 = dense[pl.ds(at + 1, 16), :]
            acc = None
            for k in range(weight.shape[1]):
                moved = pltpu.roll(jnp.where(lane < b + k, x1, x0).astype(jnp.bfloat16), 128 - b - k, 1)
                term = weight[big, k] * moved.astype(jnp.float32)
                acc = term if acc is None else acc + term
            done = acc.astype(jnp.bfloat16)
            sent[i, p, pl.ds(pl.multiple_of(big * 16, 16), 16), :] = done
            wide = done.astype(jnp.float32)
            power = power + wide * wide
        return power

    def parcel(c, i):
        at = pl.ds(cuts[c] * 16, (cuts[c + 1] - cuts[c]) * 16)
        peer = send_order(me, count, i)
        return pltpu.make_async_remote_copy(
            src_ref=sent.at[i, :, at, :],
            dst_ref=got.at[me, :, at, :],
            send_sem=send_sem.at[c, i],
            recv_sem=recv_sem.at[c, me],
            device_id={"az": peer},
        )

    tails = (jnp.zeros((blocks, 128), jnp.float32),) * 2
    power = jnp.zeros((16, 128), jnp.float32)
    half = count // 2
    far, near_half, own_half = (0, half // 2), (half // 2, half), (half, blocks)

    def post(c, lines_at):
        def body(i, carry):
            parcel(c, i).start()
            return carry

        lax.fori_loop(lines_at[0], min(lines_at[1], count - 1), body, 0)

    def lines_of(c, lines_at, power, send):
        low, high = lines_at
        step = math.gcd(high - low, TOGETHER)

        def group(g, power):
            held_lines = [low + g * step + u for u in range(step)]
            for big in range(cuts[c], cuts[c + 1]):
                for i in held_lines:
                    power = filtered(i, big, power)
            if send:
                for i in held_lines:

                    @pl.when(i < count - 1)
                    def _(i=i):
                        parcel(c, i).start()

            return power

        return lax.fori_loop(0, (high - low) // step, group, power)

    for c in range(chunks):
        for copy, sends, receives in halo[2 * c : 2 * c + 2]:
            finish(copy, sends, receives)
        for first_tile in range(bounds[c], bounds[c + 1], WIDE):
            tails = azimuth(first_tile, min(WIDE, bounds[c + 1] - first_tile), tails)
        if c == chunks - 1:
            for p in range(2):
                ends = jnp.where(lane_row < 64, tails[p], 0.0)
                dense[pl.ds(p * blocks * span + tiles, blocks, stride=span), :] = ends
        power = lines_of(c, far, power, True)
        if c < chunks - 1:
            power = lines_of(c, own_half, power, True)
            power = lines_of(c, near_half, power, True)
    c = chunks - 1
    power = lines_of(c, near_half, power, False)
    power = lines_of(c, own_half, power, False)

    own_power = jnp.broadcast_to(jnp.sum(power, keepdims=True), (1, 128))
    have = jnp.int32(0)
    for j in range(blocks):
        have = have + jnp.maximum(
            jnp.minimum(high_edge[j], cols) - jnp.maximum(low_edge[j], 0), 0
        )
    own_count = jnp.full((1, 128), have, jnp.int32).astype(jnp.float32)
    lane_note = lax.broadcasted_iota(jnp.int32, (1, 128), 1)
    stats = jnp.where(lane_note == 127, own_power, own_count)
    for i in range(blocks):
        place = jnp.full((1, 128), dest[lines[i]] % blocks, jnp.int32).astype(jnp.float32)
        memo[i] = jnp.where(lane_note < 126, place, stats)

    def told(i):
        return pltpu.make_async_remote_copy(
            src_ref=memo.at[i],
            dst_ref=notes.at[me],
            send_sem=note_send.at[i],
            recv_sem=note_recv.at[me],
            device_id={"az": send_order(me, count, i)},
        )

    def tell(i, carry):
        told(i).start()
        return carry

    lax.fori_loop(0, count - 1, tell, 0)
    post(chunks - 1, own_half)
    post(chunks - 1, near_half)
    notes[me] = memo[blocks - 1]
    got[me] = sent[blocks - 1]

    for c in range(chunks):
        lo, wide = cuts[c] * 16, (cuts[c + 1] - cuts[c]) * 16
        at = pl.ds(lo, wide)

        def take(i, carry):
            peer = send_order(me, count, i)
            parcel(c, i).wait_send()
            pltpu.make_async_remote_copy(
                src_ref=sent.at[i, :, at, :],
                dst_ref=got.at[peer, :, at, :],
                send_sem=send_sem.at[c, i],
                recv_sem=recv_sem.at[c, peer],
                device_id={"az": peer},
            ).wait_recv()
            return carry

        lax.fori_loop(0, count - 1, take, 0)

        def spread(s, carry):
            for p in range(2):
                dense[pl.ds((p * blocks + s) * span + lo, wide), :] = got[s, p, at, :].astype(jnp.float32)
            return carry

        lax.fori_loop(0, blocks, spread, 0)
        for t in range(lo, lo + wide):
            for p in range(2):
                x = dense[pl.ds(p * blocks * span + t, blocks, stride=span), :]
                nat[p, :, t * 128 : t * 128 + 128] = x.astype(jnp.bfloat16)

    def hear(i, carry):
        peer = send_order(me, count, i)
        told(i).wait_send()
        pltpu.make_async_remote_copy(
            src_ref=memo.at[i],
            dst_ref=notes.at[peer],
            send_sem=note_send.at[i],
            recv_sem=note_recv.at[peer],
            device_id={"az": peer},
        ).wait_recv()
        return carry

    lax.fori_loop(0, count - 1, hear, 0)


def finish_kernel(total, parts, nat, notes, out, mean, share, scaled, figures, done):
    blocks, cols = out.shape[1], out.shape[2]
    told = [notes[s] for s in range(blocks)]
    both = functools.reduce(lambda a, b: a + b, told)
    power, count = both[:, 127:128], both[:, 126:127]
    mean_power = power / jnp.maximum(count, 1.0)
    gain = lax.rsqrt(mean_power + 0.5)
    lane = lax.broadcasted_iota(jnp.int32, (1, 128), 1)
    place = functools.reduce(
        lambda a, s: jnp.where(lane == s, told[s], a), range(blocks), jnp.full((1, 128), -1.0)
    )
    row = lax.broadcasted_iota(jnp.int32, (blocks, 128), 0).astype(jnp.float32)
    pick = (row == place).astype(jnp.float32).astype(jnp.bfloat16)[:, :blocks]
    figures[0, 0] = mean_power[0, 0]
    figures[1, 0] = (count / float(total))[0, 0]
    copies = [
        pltpu.make_async_copy(figures.at[k], target, done.at[k]) for k, target in enumerate((mean, share))
    ]
    for copy in copies:
        copy.start()
    piece = cols // parts
    for c in range(parts):
        for p in range(2):
            for t in range(c * piece, (c + 1) * piece, 1024):
                wide = min(1024, (c + 1) * piece - t)
                x = jnp.dot(pick, nat[p, :, t : t + wide], preferred_element_type=jnp.float32)
                scaled[p, :, t : t + wide] = (x * gain).astype(jnp.bfloat16)
            at = pl.ds(c * piece, piece)
            copy = pltpu.make_async_copy(
                scaled.at[p, :, at], out.at[p, :, at], done.at[2 + 2 * c + p]
            )
            copy.start()
            copies.append(copy)
    for copy in copies:
        copy.wait()


def shards(
    secondary, line_valid, first_valid, last_valid, az_coef, az_base, rg_base, rg_coef, block_dest
):
    cols = secondary.shape[2]
    blocks = block_dest.shape[0]
    tiles = cols // 128
    count = lax.axis_size("az")
    bigs = tiles // 16
    cuts = [0] + sorted({bigs * cut // 6 for cut in CUTS} - {0, bigs}) + [bigs]
    chunks = len(cuts) - 1
    parts = max(c for c in range(1, PARTS + 1) if bigs % c == 0)
    vmem = pl.BlockSpec(memory_space=pltpu.VMEM)
    held = blocks + 2 * HALO
    dma = pltpu.SemaphoreType.DMA
    stages = max(1, (-(-count // NEAR)).bit_length())
    nat, notes = pl.pallas_call(
        functools.partial(swath_kernel, cuts),
        out_shape=(
            pltpu.VMEM((2, blocks, cols), jnp.bfloat16),
            pltpu.VMEM((blocks, 1, 128), jnp.float32),
        ),
        in_specs=[pl.BlockSpec(memory_space=pl.ANY)] * 9,
        out_specs=(vmem, vmem),
        scratch_shapes=[
            pltpu.SMEM(rg_coef.shape, jnp.float32),
            pltpu.SMEM((blocks,), jnp.int32),
            pltpu.SMEM((blocks,), jnp.int32),
            pltpu.SMEM((blocks,), jnp.int32),
            pltpu.SMEM((blocks,), jnp.int32),
            pltpu.SMEM((blocks,), jnp.int32),
            pltpu.SMEM(az_coef.shape, jnp.float32),
            pltpu.SMEM((blocks,), jnp.int32),
            pltpu.VMEM((2, held, cols), jnp.bfloat16),
            pltpu.VMEM((2, held, 128), jnp.float32),
            pltpu.VMEM((2 * blocks * (tiles + 8), 128), jnp.float32),
            pltpu.VMEM((cols // GROUP, range_taps(cols), GROUP // 128, 128), jnp.float32),
            pltpu.VMEM((blocks, 2, tiles, 128), jnp.bfloat16),
            pltpu.VMEM((blocks, 2, tiles, 128), jnp.bfloat16),
            pltpu.VMEM((blocks, 1, 128), jnp.float32),
            pltpu.SMEM((cols // GROUP,), jnp.int32),
            pltpu.SMEM((blocks,), jnp.int32),
            pltpu.SemaphoreType.REGULAR((stages,)),
            dma((8,)),
            dma(()),
            dma((chunks, 2)),
            dma((chunks, 2)),
            dma((2,)),
            dma((2,)),
            dma((chunks, blocks)),
            dma((chunks, blocks)),
            dma((blocks,)),
            dma((blocks,)),
        ],
        compiler_params=pltpu.CompilerParams(collective_id=0, has_side_effects=True),
        name="swath",
    )(
        rg_coef, rg_base, block_dest, line_valid, first_valid, last_valid, az_coef, az_base,
        secondary,
    )
    return pl.pallas_call(
        functools.partial(finish_kernel, cols * blocks * count, parts),
        out_shape=(
            jax.ShapeDtypeStruct((2, blocks, cols), jnp.bfloat16),
            jax.ShapeDtypeStruct((1,), jnp.float32),
            jax.ShapeDtypeStruct((1,), jnp.float32),
        ),
        in_specs=[vmem, vmem],
        out_specs=(pl.BlockSpec(memory_space=pl.ANY),) * 3,
        scratch_shapes=[
            pltpu.VMEM((2, blocks, cols), jnp.bfloat16),
            pltpu.SMEM((2, 1), jnp.float32),
            dma((2 + 2 * parts,)),
        ],
        name="finish",
    )(
        pltpu.with_memory_space_constraint(nat, pltpu.VMEM),
        pltpu.with_memory_space_constraint(notes, pltpu.VMEM),
    )


CUTS = (1, 3)
PARTS = 2
TOGETHER = 4
NEAR = 4
WIDE = 9


def solution(mesh):
    rows = P(("scene", "az"))
    placed = (
        P(None, ("scene", "az"), None),
        rows,
        rows,
        rows,
        P(None, ("scene", "az")),
        rows,
        rows,
        P("scene"),
        rows,
    )
    return jax.shard_map(
        shards,
        mesh=mesh,
        in_specs=placed,
        out_specs=(P(None, ("scene", "az"), None), P("scene"), P("scene")),
        check_vma=False,
    )
```

```python
import functools
import math

import jax
import jax.numpy as jnp
from jax import lax
from jax.experimental import pallas as pl
from jax.experimental.pallas import tpu as pltpu
from jax.sharding import PartitionSpec as P

HALO = 8
GROUP = 2048
RANGE_LIMIT = 3.0
NOTE = 8
PI = 3.141592653589793
HALF = 0.7071067811865476
COS8 = (1.0, HALF, 0.0, -HALF, -1.0, -HALF, 0.0, HALF)


def range_spread(cols):
    half = GROUP / 2 / cols
    return RANGE_LIMIT * (half + 1.0 - (1.0 - half) ** 2 + 1.0 - (1.0 - half) ** 3) + 0.03


def range_taps(cols):
    return math.ceil(2.0 * (4.0 + range_spread(cols)))


def range_weights(coef, start, weight, cols):
    reach = 4.0 + range_spread(cols)
    for g in range(cols // GROUP):
        centre = (g + 0.5) * GROUP / cols
        oc = coef[0] + coef[1] * centre + coef[2] * (centre * centre) + coef[3] * (centre**3)
        n0 = (oc - reach + 64.0).astype(jnp.int32) - 63
        start[g] = n0
        sub = lax.broadcasted_iota(jnp.int32, (GROUP // 128, 128), 0)
        lane = lax.broadcasted_iota(jnp.int32, (GROUP // 128, 128), 1)
        col = g * GROUP + sub * 128 + lane
        v = (col.astype(jnp.float32) + 0.5) / cols
        off = coef[0] + coef[1] * v + coef[2] * v * v + coef[3] * v * v * v
        whole = jnp.round(off)
        part = off - whole
        odd = (whole.astype(jnp.int32) + n0) & 1
        sine = jnp.sin(PI * part) * (-1.0 / PI) * (1 - 2 * odd).astype(jnp.float32)
        base = (n0.astype(jnp.float32) - off) * (PI / 4.0)
        c0, s0 = jnp.cos(base), jnp.sin(base)
        for k in range(weight.shape[1]):
            n = n0 + k
            d = n.astype(jnp.float32) - off
            ck, sk = COS8[k % 8], COS8[(k - 2) % 8]
            taper = 0.5 + 0.5 * (c0 * ck - s0 * sk)
            top = sine if k % 2 == 0 else -sine
            near = d == 0.0
            val = jnp.where(near, 1.0, top / jnp.where(near, 1.0, d)) * taper
            keep = (jnp.abs(d) < 4.0) & (col + n >= 0) & (col + n < cols)
            val = jnp.where(keep, val, 0.0)
            weight[g, k] = val.astype(jnp.bfloat16).astype(jnp.float32)


def column(values):
    row = lax.broadcasted_iota(jnp.int32, (len(values), 128), 0)
    made = jnp.zeros((len(values), 128), jnp.asarray(values[0]).dtype)
    for r, value in enumerate(values):
        made = jnp.where(row == r, value, made)
    return made


def azimuth_band(fraction, base, line, blocks):
    held = lax.broadcasted_iota(jnp.int32, (blocks, 128), 1)
    row = jnp.where(held < blocks, held, held - blocks - HALO)
    row = jnp.where(held < blocks + HALO, row, held - HALO)
    gap = row - line - base
    d = gap.astype(jnp.float32) - fraction
    near = d == 0.0
    safe = jnp.where(near, 1.0, d)
    whole = jnp.round(safe)
    sine = jnp.sin(PI * (safe - whole)) * (1 - 2 * (whole.astype(jnp.int32) & 1)).astype(jnp.float32)
    value = jnp.where(near, 1.0, sine / (PI * safe)) * (0.5 + 0.5 * jnp.cos(PI * d / 4.0))
    keep = (jnp.abs(d) < 4.0) & (jnp.abs(gap) <= 4) & (held < blocks + 2 * HALO)
    return jnp.where(keep, value, 0.0).astype(jnp.bfloat16)


def send_order(me, count, i):
    half = count // 2
    mine = me // half
    local = me - mine * half
    slot = jnp.where(mine == 1, i, lax.rem(i + half, count - 1))
    slot = jnp.where(i == count - 1, i, slot)
    own = slot // half
    side = mine * own + (1 - mine) * (1 - own)
    near = lax.rem(local + own + slot - own * half, half)
    if half % 2:
        return side * half + near
    quarter = half // 2
    group = slot // quarter
    far = (mine * group + (1 - mine) * (1 - group)) * quarter + lax.rem(me + slot, quarter)
    return side * half + jnp.where(own == 1, near, far)


def swath_kernel(
    cuts, coef_in, shift_in, dest_in, valid_in, first_in, last_in, az_coef_in, az_base_in, image,
    nat, notes,
    coef, shift, dest, valid, first, last, az_coef, az_base,
    held, edge, dense, weight, sent, got, memo, start, order,
    ready, load_sem, own_sem, halo_send, halo_recv, edge_send, edge_recv, send_sem, recv_sem, note_send, note_recv,
):
    blocks, cols = image.shape[1], image.shape[2]
    tiles = cols // 128
    span = dense.shape[0] // (2 * blocks)
    count = lax.axis_size("az")
    me = lax.axis_index("az")
    after, before = lax.rem(me + 1, count), lax.rem(me + count - 1, count)
    up, down = me < count - 1, me > 0

    barrier = pltpu.get_barrier_semaphore()
    near = min(NEAR, count - 1)

    def greet(semaphore, step):
        @pl.when(me + step < count)
        def _():
            pl.semaphore_signal(semaphore, inc=1, device_id={"az": lax.rem(me + step, count)})

        @pl.when(me >= step)
        def _():
            pl.semaphore_signal(semaphore, inc=1, device_id={"az": lax.rem(me + count - step, count)})

    for step in range(1, near + 1):
        greet(barrier, step)
    own = pltpu.make_async_copy(image, held.at[:, pl.ds(0, blocks)], own_sem)
    own.start()
    loads = [
        pltpu.make_async_copy(source, target, load_sem.at[k])
        for k, (source, target) in enumerate(
            (
                (valid_in, valid), (first_in, first), (last_in, last), (coef_in, coef),
                (shift_in, shift), (dest_in, dest), (az_coef_in, az_coef), (az_base_in, az_base),
            )
        )
    ]
    for load in loads:
        load.start()
    for load in loads:
        load.wait()
    low_edge = [jnp.where(valid[r] > 0, first[r], cols) for r in range(blocks)]
    high_edge = [jnp.where(valid[r] > 0, last[r], 0) for r in range(blocks)]
    edge[0, pl.ds(0, blocks), :] = column(low_edge).astype(jnp.float32)
    edge[1, pl.ds(0, blocks), :] = column(high_edge).astype(jnp.float32)
    own.wait()
    pl.semaphore_wait(barrier, jnp.minimum(me, near) + jnp.minimum(count - 1 - me, near))

    chunks = len(cuts) - 1
    bounds = [0] + [cut * 16 + 1 for cut in cuts[1:-1]] + [tiles]
    ways = ((after, blocks - HALO, blocks, up, down), (before, 0, blocks + HALO, down, up))

    def begin(copy, sends):
        @pl.when(sends)
        def _():
            copy.start()

    def finish(copy, sends, receives):
        @pl.when(sends)
        def _():
            copy.wait_send()

        @pl.when(receives)
        def _():
            copy.wait_recv()

    halo = []
    for c in range(chunks):
        at = pl.ds(bounds[c] * 128, (bounds[c + 1] - bounds[c]) * 128)
        for w, (peer, source, slot, sends, receives) in enumerate(ways):
            copy = pltpu.make_async_remote_copy(
                src_ref=held.at[:, pl.ds(source, HALO), at],
                dst_ref=held.at[:, pl.ds(slot, HALO), at],
                send_sem=halo_send.at[c, w],
                recv_sem=halo_recv.at[c, w],
                device_id={"az": peer},
            )
            begin(copy, sends)
            halo.append((copy, sends, receives))
        if c == 0:
            bounds_sent = []
            for w, (peer, source, slot, sends, receives) in enumerate(ways):
                copy = pltpu.make_async_remote_copy(
                    src_ref=edge.at[:, pl.ds(source, HALO), :],
                    dst_ref=edge.at[:, pl.ds(slot, HALO), :],
                    send_sem=edge_send.at[w],
                    recv_sem=edge_recv.at[w],
                    device_id={"az": peer},
                )
                begin(copy, sends)
                bounds_sent.append((copy, sends, receives))

    reach = near
    stage = 0
    if reach < count - 1:
        greet(ready.at[0], reach)

    lines = []
    for i in range(blocks):
        target = send_order(me, count, i)
        line = jnp.int32(0)
        for j in range(blocks):
            line = jnp.where(dest[j] // blocks == target, j, line)
        order[i] = line
        lines.append(line)
    c0 = column([az_coef[0, j] for j in lines])
    c1 = column([az_coef[1, j] for j in lines])
    c2 = column([az_coef[2, j] for j in lines])
    q = 0.5
    fraction = c0 + c1 * q + c2 * q * q
    band = azimuth_band(fraction, column([az_base[j] for j in lines]), column(lines), blocks)
    band = band[:, : blocks + 2 * HALO]
    range_weights(coef, start, weight, cols)
    while reach < count - 1:
        pl.semaphore_wait(
            ready.at[stage], (me >= reach).astype(jnp.int32) + (me + reach < count).astype(jnp.int32)
        )
        reach, stage = 2 * reach, stage + 1
        if reach < count - 1:
            greet(ready.at[stage], reach)

    for copy, sends, receives in bounds_sent:
        finish(copy, sends, receives)
    low = edge[0]
    high = edge[1]
    row = lax.broadcasted_iota(jnp.int32, high.shape, 0)
    outside = ((me == 0) & (row >= blocks) & (row < blocks + HALO)) | (
        (me == count - 1) & (row >= blocks + HALO)
    )
    high = jnp.where(outside, 0.0, high)
    lane_held = lax.broadcasted_iota(jnp.int32, high.shape, 1).astype(jnp.float32)
    lane_row = lax.broadcasted_iota(jnp.int32, (blocks, 128), 1)
    lane = lax.broadcasted_iota(jnp.int32, (16, 128), 1)

    def azimuth(first_tile, wide, tails):
        at = pl.ds(first_tile * 128, wide * 128)
        keeps = []
        for u in range(wide):
            col = lane_held + ((first_tile + u) * 128.0)
            keeps.append((col >= low) & (col < high))
        new_tails = []
        for p in range(2):
            rows = held[p, :, at].astype(jnp.float32)
            rows = jnp.concatenate(
                [
                    jnp.where(keep, rows[:, u * 128 : u * 128 + 128], 0.0)
                    for u, keep in enumerate(keeps)
                ],
                axis=1,
            ).astype(jnp.bfloat16)
            out = jnp.dot(band, rows, preferred_element_type=jnp.float32)
            out = out.astype(jnp.bfloat16).astype(jnp.float32)
            tail = tails[p]
            for u in range(wide):
                turned = pltpu.roll(out[:, u * 128 : u * 128 + 128], 64, 1)
                place = p * blocks * span + first_tile + u
                dense[pl.ds(place, blocks, stride=span), :] = jnp.where(lane_row < 64, tail, turned)
                tail = turned
            new_tails.append(tail)
        return tuple(new_tails)

    def filtered(i, big, power):
        b = shift[order[i]] + start[big] + 64
        for p in range(2):
            at = pl.multiple_of((p * blocks + i) * span + big * 16, 8)
            x0 = dense[pl.ds(at, 16), :]
            x1 = dense[pl.ds(at + 1, 16), :]
            acc = None
            for k in range(weight.shape[1]):
                moved = pltpu.roll(jnp.where(lane < b + k, x1, x0).astype(jnp.bfloat16), 128 - b - k, 1)
                term = weight[big, k] * moved.astype(jnp.float32)
                acc = term if acc is None else acc + term
            done = acc.astype(jnp.bfloat16)
            sent[i, p, pl.ds(pl.multiple_of(big * 16, 16), 16), :] = done
            wide = done.astype(jnp.float32)
            power = power + wide * wide
        return power

    def parcel(c, i):
        at = pl.ds(cuts[c] * 16, (cuts[c + 1] - cuts[c]) * 16)
        peer = send_order(me, count, i)
        return pltpu.make_async_remote_copy(
            src_ref=sent.at[i, :, at, :],
            dst_ref=got.at[me, :, at, :],
            send_sem=send_sem.at[c, i],
            recv_sem=recv_sem.at[c, me],
            device_id={"az": peer},
        )

    tails = (jnp.zeros((blocks, 128), jnp.float32),) * 2
    power = jnp.zeros((16, 128), jnp.float32)
    half = count // 2
    far, near_half, own_half = (0, half // 2), (half // 2, half), (half, blocks)

    def post(c, lines_at):
        def body(i, carry):
            parcel(c, i).start()
            return carry

        lax.fori_loop(lines_at[0], min(lines_at[1], count - 1), body, 0)

    def lines_of(c, lines_at, power, send):
        low, high = lines_at
        step = math.gcd(high - low, TOGETHER)

        def group(g, power):
            held_lines = [low + g * step + u for u in range(step)]
            for big in range(cuts[c], cuts[c + 1]):
                for i in held_lines:
                    power = filtered(i, big, power)
            if send:
                for i in held_lines:

                    @pl.when(i < count - 1)
                    def _(i=i):
                        parcel(c, i).start()

            return power

        return lax.fori_loop(0, (high - low) // step, group, power)

    for c in range(chunks):
        for copy, sends, receives in halo[2 * c : 2 * c + 2]:
            finish(copy, sends, receives)
        for first_tile in range(bounds[c], bounds[c + 1], WIDE):
            tails = azimuth(first_tile, min(WIDE, bounds[c + 1] - first_tile), tails)
        if c == chunks - 1:
            for p in range(2):
                ends = jnp.where(lane_row < 64, tails[p], 0.0)
                dense[pl.ds(p * blocks * span + tiles, blocks, stride=span), :] = ends
        power = lines_of(c, far, power, True)
        if c < chunks - 1:
            power = lines_of(c, own_half, power, True)
            power = lines_of(c, near_half, power, True)
    c = chunks - 1
    power = lines_of(c, near_half, power, False)
    power = lines_of(c, own_half, power, False)

    own_power = jnp.broadcast_to(jnp.sum(power, keepdims=True), (1, 128))
    have = jnp.int32(0)
    for j in range(blocks):
        have = have + jnp.maximum(
            jnp.minimum(high_edge[j], cols) - jnp.maximum(low_edge[j], 0), 0
        )
    own_count = jnp.full((1, 128), have, jnp.int32).astype(jnp.float32)
    lane_note = lax.broadcasted_iota(jnp.int32, (1, 128), 1)
    stats = jnp.where(lane_note == 127, own_power, own_count)
    for i in range(blocks):
        place = jnp.full((1, 128), dest[lines[i]] % blocks, jnp.int32).astype(jnp.float32)
        memo[i] = jnp.where(lane_note < 126, place, stats)

    def told(i):
        return pltpu.make_async_remote_copy(
            src_ref=memo.at[i],
            dst_ref=notes.at[me],
            send_sem=note_send.at[i],
            recv_sem=note_recv.at[me],
            device_id={"az": send_order(me, count, i)},
        )

    def tell(i, carry):
        told(i).start()
        return carry

    lax.fori_loop(0, count - 1, tell, 0)
    post(chunks - 1, own_half)
    post(chunks - 1, near_half)
    notes[me] = memo[blocks - 1]
    got[me] = sent[blocks - 1]

    for c in range(chunks):
        lo, wide = cuts[c] * 16, (cuts[c + 1] - cuts[c]) * 16
        at = pl.ds(lo, wide)

        def take(i, carry):
            peer = send_order(me, count, i)
            parcel(c, i).wait_send()
            pltpu.make_async_remote_copy(
                src_ref=sent.at[i, :, at, :],
                dst_ref=got.at[peer, :, at, :],
                send_sem=send_sem.at[c, i],
                recv_sem=recv_sem.at[c, peer],
                device_id={"az": peer},
            ).wait_recv()
            return spread(peer, carry)

        def spread(s, carry):
            for p in range(2):
                row = pl.multiple_of((p * blocks + s) * span + lo, 8)
                dense[pl.ds(row, wide), :] = got[s, p, at, :].astype(jnp.float32)
            return carry

        spread(me, 0)
        lax.fori_loop(0, count - 1, take, 0)
        for t in range(lo, lo + wide):
            for p in range(2):
                x = dense[pl.ds(p * blocks * span + t, blocks, stride=span), :]
                nat[p, :, t * 128 : t * 128 + 128] = x.astype(jnp.bfloat16)

    def hear(i, carry):
        peer = send_order(me, count, i)
        told(i).wait_send()
        pltpu.make_async_remote_copy(
            src_ref=memo.at[i],
            dst_ref=notes.at[peer],
            send_sem=note_send.at[i],
            recv_sem=note_recv.at[peer],
            device_id={"az": peer},
        ).wait_recv()
        return carry

    lax.fori_loop(0, count - 1, hear, 0)


def finish_kernel(total, parts, nat, notes, out, mean, share, scaled, figures, done):
    blocks, cols = out.shape[1], out.shape[2]
    told = [notes[s] for s in range(blocks)]
    both = functools.reduce(lambda a, b: a + b, told)
    power, count = both[:, 127:128], both[:, 126:127]
    mean_power = power / jnp.maximum(count, 1.0)
    gain = lax.rsqrt(mean_power + 0.5)
    lane = lax.broadcasted_iota(jnp.int32, (1, 128), 1)
    place = functools.reduce(
        lambda a, s: jnp.where(lane == s, told[s], a), range(blocks), jnp.full((1, 128), -1.0)
    )
    row = lax.broadcasted_iota(jnp.int32, (blocks, 128), 0).astype(jnp.float32)
    pick = (row == place).astype(jnp.float32).astype(jnp.bfloat16)[:, :blocks]
    figures[0, 0] = mean_power[0, 0]
    figures[1, 0] = (count / float(total))[0, 0]
    copies = [
        pltpu.make_async_copy(figures.at[k], target, done.at[k]) for k, target in enumerate((mean, share))
    ]
    for copy in copies:
        copy.start()
    piece = cols // parts
    for c in range(parts):
        for p in range(2):
            for t in range(c * piece, (c + 1) * piece, 1024):
                wide = min(1024, (c + 1) * piece - t)
                x = jnp.dot(pick, nat[p, :, t : t + wide], preferred_element_type=jnp.float32)
                scaled[p, :, t : t + wide] = (x * gain).astype(jnp.bfloat16)
            at = pl.ds(c * piece, piece)
            copy = pltpu.make_async_copy(
                scaled.at[p, :, at], out.at[p, :, at], done.at[2 + 2 * c + p]
            )
            copy.start()
            copies.append(copy)
    for copy in copies:
        copy.wait()


def shards(
    secondary, line_valid, first_valid, last_valid, az_coef, az_base, rg_base, rg_coef, block_dest
):
    cols = secondary.shape[2]
    blocks = block_dest.shape[0]
    tiles = cols // 128
    count = lax.axis_size("az")
    bigs = tiles // 16
    cuts = [0] + sorted({bigs * cut // 6 for cut in CUTS} - {0, bigs}) + [bigs]
    chunks = len(cuts) - 1
    parts = max(c for c in range(1, PARTS + 1) if bigs % c == 0)
    vmem = pl.BlockSpec(memory_space=pltpu.VMEM)
    held = blocks + 2 * HALO
    dma = pltpu.SemaphoreType.DMA
    stages = max(1, (-(-count // NEAR)).bit_length())
    nat, notes = pl.pallas_call(
        functools.partial(swath_kernel, cuts),
        out_shape=(
            pltpu.VMEM((2, blocks, cols), jnp.bfloat16),
            pltpu.VMEM((blocks, 1, 128), jnp.float32),
        ),
        in_specs=[pl.BlockSpec(memory_space=pl.ANY)] * 9,
        out_specs=(vmem, vmem),
        scratch_shapes=[
            pltpu.SMEM(rg_coef.shape, jnp.float32),
            pltpu.SMEM((blocks,), jnp.int32),
            pltpu.SMEM((blocks,), jnp.int32),
            pltpu.SMEM((blocks,), jnp.int32),
            pltpu.SMEM((blocks,), jnp.int32),
            pltpu.SMEM((blocks,), jnp.int32),
            pltpu.SMEM(az_coef.shape, jnp.float32),
            pltpu.SMEM((blocks,), jnp.int32),
            pltpu.VMEM((2, held, cols), jnp.bfloat16),
            pltpu.VMEM((2, held, 128), jnp.float32),
            pltpu.VMEM((2 * blocks * (tiles + 8), 128), jnp.float32),
            pltpu.VMEM((cols // GROUP, range_taps(cols), GROUP // 128, 128), jnp.float32),
            pltpu.VMEM((blocks, 2, tiles, 128), jnp.bfloat16),
            pltpu.VMEM((blocks, 2, tiles, 128), jnp.bfloat16),
            pltpu.VMEM((blocks, 1, 128), jnp.float32),
            pltpu.SMEM((cols // GROUP,), jnp.int32),
            pltpu.SMEM((blocks,), jnp.int32),
            pltpu.SemaphoreType.REGULAR((stages,)),
            dma((8,)),
            dma(()),
            dma((chunks, 2)),
            dma((chunks, 2)),
            dma((2,)),
            dma((2,)),
            dma((chunks, blocks)),
            dma((chunks, blocks)),
            dma((blocks,)),
            dma((blocks,)),
        ],
        compiler_params=pltpu.CompilerParams(collective_id=0, has_side_effects=True),
        name="swath",
    )(
        rg_coef, rg_base, block_dest, line_valid, first_valid, last_valid, az_coef, az_base,
        secondary,
    )
    return pl.pallas_call(
        functools.partial(finish_kernel, cols * blocks * count, parts),
        out_shape=(
            jax.ShapeDtypeStruct((2, blocks, cols), jnp.bfloat16),
            jax.ShapeDtypeStruct((1,), jnp.float32),
            jax.ShapeDtypeStruct((1,), jnp.float32),
        ),
        in_specs=[vmem, vmem],
        out_specs=(pl.BlockSpec(memory_space=pl.ANY),) * 3,
        scratch_shapes=[
            pltpu.VMEM((2, blocks, cols), jnp.bfloat16),
            pltpu.SMEM((2, 1), jnp.float32),
            dma((2 + 2 * parts,)),
        ],
        name="finish",
    )(
        pltpu.with_memory_space_constraint(nat, pltpu.VMEM),
        pltpu.with_memory_space_constraint(notes, pltpu.VMEM),
    )


CUTS = (1, 3)
PARTS = 2
TOGETHER = 4
NEAR = 4
WIDE = 9


def solution(mesh):
    rows = P(("scene", "az"))
    placed = (
        P(None, ("scene", "az"), None),
        rows,
        rows,
        rows,
        P(None, ("scene", "az")),
        rows,
        rows,
        P("scene"),
        rows,
    )
    return jax.shard_map(
        shards,
        mesh=mesh,
        in_specs=placed,
        out_specs=(P(None, ("scene", "az"), None), P("scene"), P("scene")),
        check_vma=False,
    )
```
